32 devices in a mesh: tm: 4 (over y, core), lat: 8 (over z, x).
Axes of the slice: x: 2, y: 2, z: 4, core: 2. Of those that a mesh axis runs over, the one named last changes fastest.
Arguments:
- trajectory: float32 [4, 32, 64, 2048], P('tm', 'lat'), may hold values from -6 to 6
- diffusivity: float32 [4, 32, 64, 2048], P('tm', 'lat'), may hold values from 0.02 to 0.24
- adjoint_end: bfloat16 [32, 64, 2048], P('lat'), may hold values from -6 to 6
- obs_jac: bfloat16 [3072, 128, 128], P(('tm', 'lat')), may hold values from -0.5 to 0.5
- obs_value: float32 [3072, 128], P(('tm', 'lat')), may hold values from -6 to 6
- obs_weight: float32 [3072, 128], P(('tm', 'lat')), may hold values from 0.3 to 3
- obs_valid: int32 [3072, 128], P(('tm', 'lat')), may hold values 0 or 1
- obs_owner: int32 [3072, 1], P(('tm', 'lat')), may hold values from 0 to 31; in each aligned block of 96 rows (0 to 95, 96 to 191, ...) at most 6 rows name the same one
- obs_tile: int32 [3072], P(('tm', 'lat')), may hold values from 0 to 4095
Outputs:
- adjoint: float32 [4, 32, 64, 2048], P('tm', 'lat')
The draws below stay inside these ranges and needn't reach their ends.
Inputs may be any that keep to these rules, and one draw needn't show every extreme that they name: `obs_owner`: among the 96 blocks of one device, no owner is named more than 6 times, a bound that some block reaches.
All inputs are finite; a program needn't handle non-finite values. No bound on the sum of `obs_valid` on one device may be relied on, other than what follows from the above.
Results may differ from the reference program's by a relative error of at most 0.0024.
Values may be sent and summed in bfloat16 or wider, within the bound.
A program may use at most 128 MiB of HBM per device.

```python
import math
import jax
import jax.numpy as jnp
import numpy as np
from jax import lax

NLON = 2048
LEV = 64
TW = 2
CH = 128
SUB = 2
NB_DEV = 96
SECTIONS = 4
NLAT = 32
TILE = 128
TILES_DEV = 4096
CAP = 6
NOBS = 3072
N_LAT = 8
DEVICES = 32


def with_ends(entries, key, smallest, high):
    shape = entries.shape
    place = [jax.random.randint(jax.random.fold_in(key, axis), (), 0, shape[axis]) for axis in range(len(shape))]
    entries = entries.at[tuple(place)].set(smallest)
    longest = shape.index(max(shape))
    place[longest] = (place[longest] + 1) % shape[longest]
    return entries.at[tuple(place)].set(high)


def block_levels(rng, shape, cuts, least, largest):
    def one(dim, parts):
        draws = jax.random.uniform(jax.random.fold_in(jax.random.fold_in(rng, 6), dim), (parts,), jnp.float32, least / len(cuts), largest / len(cuts))
        return jnp.repeat(jnp.exp(draws), shape[dim] // parts).reshape((-1,) + (1,) * (len(shape) - dim - 1))

    loudness = one(*cuts[0])
    for cut in cuts[1:]:
        loudness = loudness * one(*cut)
    return loudness


def deal_out(key, own, number, rows, count, top, most, lean):
    sequence = jax.random.permutation(key, count)
    packed, ordinary = load_shares(count, rows * top, most, lean, True), load_shares(count, rows * top, most, lean, False)
    places = jnp.arange(count)

    def named(tallies, rotation):
        used = int((tallies > 0).sum())
        fixed = max(1, used // 4)
        shifted = fixed + (places - fixed + rotation * (used - fixed)) % max(1, count - fixed)
        return jnp.zeros((count,), jnp.int32).at[sequence[jnp.where(places < fixed, places, shifted)]].set(jnp.asarray(tallies, jnp.int32))

    tallies = jnp.where(number % 4 == 0, named(packed, number // 4), named(ordinary, number - number // 4 - 1))
    mixed = jax.random.permutation(jax.random.fold_in(own, 3), count)
    source_of, sink = mixed[0:count // 2 * 2:2], mixed[1:count // 2 * 2:2]
    slack = jnp.minimum(tallies[source_of] - 1, most - tallies[sink]) // 2
    slack = jnp.where((source_of == sequence[0]) | (sink == sequence[0]) | (tallies[sink] == 0), 0, jnp.maximum(slack, 0))
    shifted = jax.random.randint(jax.random.fold_in(own, 4), (count // 2,), 0, 1 << 20) % (slack + 1)
    tallies = tallies.at[source_of].add(-shifted).at[sink].add(shifted)
    labels = jnp.searchsorted(jnp.cumsum(tallies), jnp.arange(rows * top), side="right").astype(jnp.int32)
    grid = labels.reshape(top, rows).T
    grid = grid[jax.random.permutation(jax.random.fold_in(own, 1), rows)]
    rotation = jax.random.randint(jax.random.fold_in(own, 2), (rows, 1), 0, top)
    return jnp.take_along_axis(grid, (jnp.arange(top)[None, :] + rotation) % top, axis=1)


def load_shares(amount, total, most, slope, full):
    weights = [(1 << 20) // math.isqrt(standing ** slope) + 1 for standing in range(1, amount + 1)]
    largest = most if full else min(most, max(-(-total // amount), total * weights[0] // sum(weights)))
    least = 1 if total - largest >= amount - 1 else 0
    counts, surplus = [largest] + [least] * (amount - 1), total - largest - least * (amount - 1)
    while surplus > 0:
        movable = [i for i in range(1, amount) if counts[i] < largest] or [i for i in range(1, amount) if counts[i] < most]
        mass, remaining = sum([weights[i] for i in movable]), surplus
        for i in movable:
            more = min(most - counts[i], max(1, remaining * weights[i] // mass), surplus)
            counts[i] = counts[i] + more
            surplus = surplus - more
    return np.array(counts)


def gaussian(rng, shape, scale, most, shards=(), held_as=jnp.bfloat16):
    level = block_levels(rng, shape, shards, -0.22, 0.18) if shards else 1.0
    result = jax.random.normal(rng, shape, jnp.float32) * scale * level
    return jnp.minimum(jnp.maximum(result, -most), most).astype(held_as)


def setup_inputs(seed: int = 0) -> dict:
    streams_of = jax.random.split(jax.random.key(seed), 10)
    trajectory = gaussian(streams_of[0], (SECTIONS, NLAT, LEV, NLON), 1.0, 6.0, ((0, 4), (1, 8)), jnp.float32)
    diffusivity = jnp.clip(jnp.exp(math.log(0.24) - 2.4849066 * jax.random.uniform(streams_of[1], (SECTIONS, NLAT, LEV, NLON), jnp.float32) ** block_levels(streams_of[1], (SECTIONS, NLAT, LEV, NLON), ((0, 4), (1, 8)), -0.2, 0.2)), 0.02, 0.24)
    adjoint_end = gaussian(streams_of[2], (NLAT, LEV, NLON), 1.0, 6.0, ((0, 8),))
    obs_jac = gaussian(streams_of[3], (NOBS, CH, TILE), TILE ** -0.5, 0.5, ((0, 32),))
    obs_value = gaussian(streams_of[4], (NOBS, CH), 1.0, 6.0, ((0, 32),), jnp.float32)
    obs_weight = jnp.clip(jnp.exp(math.log(3.0) - 2.3025851 * jax.random.uniform(streams_of[5], (NOBS, CH), jnp.float32) ** block_levels(streams_of[5], (NOBS, CH), ((0, 32),), -0.2, 0.2)), 0.3, 3.0)
    obs_valid = with_ends((jax.random.randint(streams_of[6], (NOBS, CH), 0, 4) < 3).astype(jnp.int32), jax.random.fold_in(streams_of[6], 1), 0, 1)
    obs_owner_keys = jax.random.split(jax.random.fold_in(streams_of[7], 1), NOBS // NB_DEV)
    obs_owner_turns = jax.random.permutation(jax.random.fold_in(streams_of[7], 3), NOBS // NB_DEV)
    obs_owner = jax.vmap(lambda own, number: deal_out(jax.random.fold_in(streams_of[7], 2), own, number, NB_DEV, DEVICES, 1, CAP, 2))(obs_owner_keys, obs_owner_turns).reshape((NOBS, 1))
    obs_tile = with_ends(jax.random.randint(streams_of[8], (NOBS,), 0, TILES_DEV), jax.random.fold_in(streams_of[8], 1), 0, TILES_DEV - 1).astype(jnp.int32)
    return dict(trajectory=trajectory, diffusivity=diffusivity, adjoint_end=adjoint_end, obs_jac=obs_jac, obs_value=obs_value, obs_weight=obs_weight, obs_valid=obs_valid, obs_owner=obs_owner, obs_tile=obs_tile)


def spread(weighted):
    padded = jnp.pad(weighted, ((1, 1), (0, 0), (0, 0)))
    return padded[2:] + padded[:-2] + jnp.roll(weighted, 1, 2) + jnp.roll(weighted, -1, 2) - 4.0 * weighted


def propagate(field, kappa):
    for _ in range(SUB):
        field = field + spread(kappa * field)
    return field


def reference(trajectory, diffusivity, adjoint_end, obs_jac, obs_value, obs_weight, obs_valid, obs_owner, obs_tile):
    per_row = NLON // TW
    tiles = trajectory.reshape(SECTIONS, NLAT, LEV, per_row, TW).transpose(0, 1, 3, 2, 4).reshape(SECTIONS * NLAT * per_row, TILE)
    owner = obs_owner[:, 0]
    section = owner // N_LAT
    band = owner % N_LAT
    flat = (section * NLAT * per_row + band * TILES_DEV + obs_tile).astype(jnp.int32)
    states = tiles[flat]
    weights = obs_weight * obs_valid.astype(jnp.float32)

    def one(args):
        jac, state, value, weight = args
        jac_f = jac.astype(jnp.float32)
        pred = jnp.einsum("bct,bt->bc", jac_f, state, precision=lax.Precision.HIGHEST)
        resid = weight * (value - pred)
        return jnp.einsum("bct,bc->bt", jac_f, resid, precision=lax.Precision.HIGHEST)

    terms = lax.map(one, (obs_jac.reshape(DEVICES, NB_DEV, CH, TILE), states.reshape(DEVICES, NB_DEV, TILE),
                          obs_value.reshape(DEVICES, NB_DEV, CH), weights.reshape(DEVICES, NB_DEV, CH)))
    terms = terms.reshape(NOBS, TILE)
    forcing = jnp.zeros((SECTIONS * NLAT * per_row, TILE), jnp.float32).at[flat].add(terms)
    forcing = forcing.reshape(SECTIONS, NLAT, per_row, LEV, TW).transpose(0, 1, 3, 2, 4).reshape(SECTIONS, NLAT, LEV, NLON)
    results = [None] * SECTIONS
    current = adjoint_end.astype(jnp.float32)
    for section_id in range(SECTIONS - 1, -1, -1):
        if section_id == SECTIONS - 1:
            incoming = adjoint_end.astype(jnp.float32)
        else:
            incoming = lax.optimization_barrier(current.astype(jnp.bfloat16)).astype(jnp.float32)
        current = forcing[section_id] + propagate(incoming, diffusivity[section_id])
        results[section_id] = current
    return jnp.stack(results)
```

```python
import functools

import jax
import jax.numpy as jnp
from jax import lax
from jax.experimental import pallas as pl
from jax.experimental.pallas import tpu as pltpu
from jax.sharding import PartitionSpec as P

TW = 2
SUB = 2
LANES = 128
PAD = 8
CHUNK = 8
MESH = pl.DeviceIdType.MESH
VMEM = pl.BlockSpec(memory_space=pltpu.VMEM)


def split(x):
    top = x.astype(jnp.bfloat16)
    return top, (x - top.astype(jnp.float32)).astype(jnp.bfloat16)


def dot(a, b):
    return jnp.dot(a, b, preferred_element_type=jnp.float32)


def iota(shape, axis):
    return lax.broadcasted_iota(jnp.int32, shape, axis)


def ones_where(mask):
    return jnp.where(mask, 1.0, 0.0)


def observe_kernel(
    lats, count, slots,
    owner_ref, tile_ref, value_ref, weight_ref, valid_ref, traj_hbm, coeff_hbm, end_hbm, jac_hbm,
    forcing_ref, low_ref, high_ref, last_low_ref, last_high_ref,
    traj, coeff, end, jac, jac_t, fields, chosen, place, place_t,
    ids_out, ids_in, state_out, state_in, term_out, term_in, state_rows, resid_rows, terms,
    first_row, final_row, edge_low, edge_high,
    load_sem, ids_send, ids_recv, state_send, state_recv, term_send, term_recv, row_send, row_recv, edge_send, edge_recv,
):
    section, band = lax.axis_index("tm"), lax.axis_index("lat")
    me = section * lats + band
    rows, levels, nlon = forcing_ref.shape
    blocks = owner_ref.shape[1]
    total = count * PAD
    columns = nlon // LANES
    per_column = LANES // TW
    tile_len = levels * TW

    loads = [
        pltpu.make_async_copy(src, dst, load_sem.at[i])
        for i, (src, dst) in enumerate(
            ((traj_hbm.at[0], traj), (coeff_hbm.at[0], coeff), (end_hbm, end), (jac_hbm, jac))
        )
    ]
    for load in loads:
        load.start()

    barrier = pltpu.get_barrier_semaphore()

    def peer(j):
        to = lax.rem(me + j, count)
        return to, (to // lats, lax.rem(to, lats))

    def greet(j, carry):
        pl.semaphore_signal(barrier, inc=1, device_id=peer(j)[1], device_id_type=MESH)
        return carry

    lax.fori_loop(1, count, greet, 0)

    def swap(out, into, send, recv):
        def outgoing(j):
            to, where = peer(j)
            return pltpu.make_async_remote_copy(
                src_ref=out.at[to], dst_ref=into.at[me], send_sem=send.at[j], recv_sem=recv.at[j],
                device_id=where, device_id_type=MESH,
            )

        def incoming(j):
            source, where = peer(count - j)
            return pltpu.make_async_remote_copy(
                src_ref=out.at[source], dst_ref=into.at[source], send_sem=send.at[j], recv_sem=recv.at[j],
                device_id=where, device_id_type=MESH,
            )

        def launch(j, carry):
            outgoing(j).start()
            return carry

        def land(j, carry):
            incoming(j).wait_recv()
            return carry

        def drain(j, carry):
            outgoing(j).wait_send()
            return carry

        def begin():
            lax.fori_loop(1, count, launch, 0)
            into[me] = out[me]

        return begin, lambda: lax.fori_loop(1, count, land, 0), lambda: lax.fori_loop(1, count, drain, 0)

    ids_begin, ids_land, ids_drain = swap(ids_out, ids_in, ids_send, ids_recv)
    state_begin, state_land, state_drain = swap(state_out, state_in, state_send, state_recv)
    term_begin, term_land, term_drain = swap(term_out, term_in, term_send, term_recv)

    owner = owner_ref[...]
    mine = owner == iota((count, blocks), 0)
    before = ones_where(iota((blocks, blocks), 0) < iota((blocks, blocks), 1)).astype(jnp.bfloat16)
    rank = dot(ones_where(mine).astype(jnp.bfloat16), before)
    target = jnp.where(mine, iota((count, blocks), 0).astype(jnp.float32) * PAD + rank, 0.0)
    slot = jnp.sum(target, axis=0, keepdims=True)
    tile = tile_ref[...]
    column = (tile // per_column + 1).astype(jnp.float32)
    inside = lax.rem(tile, per_column).astype(jnp.float32)
    lane = iota((count, LANES), 1)
    packed = jnp.zeros((count, LANES), jnp.float32)
    for s in range(slots):
        here = mine & (rank == float(s))
        for at, what in ((s, column), (PAD + s, inside)):
            found = jnp.sum(jnp.where(here, what, 0.0), axis=1, keepdims=True)
            packed = jnp.where(lane == at, found, packed)
    for d in range(count):
        ids_out[d] = packed[d : d + 1]
    pl.semaphore_wait(barrier, count - 1)
    ids_begin()

    holds = ones_where(iota((total, blocks), 0).astype(jnp.float32) == slot)
    place[...] = holds.astype(jnp.bfloat16)
    place_t[...] = holds.T.astype(jnp.bfloat16)

    for load in loads[:3]:
        load.wait()
    first_row[0] = coeff[0].astype(jnp.bfloat16)
    final_row[0] = coeff[rows - 1].astype(jnp.bfloat16)
    has_low, has_high = band > 0, band < lats - 1
    is_last = section == count // lats - 1

    def beside(src, dst, i, send, recv, shift):
        return pltpu.make_async_remote_copy(
            src_ref=src, dst_ref=dst, send_sem=send.at[i], recv_sem=recv.at[i],
            device_id=(section, band + shift), device_id_type=MESH,
        )

    def row_down():
        return beside(first_row, high_ref, 0, row_send, row_recv, -1)

    def row_up():
        return beside(final_row, low_ref, 1, row_send, row_recv, 1)

    def edge_down():
        return beside(edge_low, last_high_ref, 0, edge_send, edge_recv, -1)

    def edge_up():
        return beside(edge_high, last_low_ref, 1, edge_send, edge_recv, 1)

    @pl.when(has_low)
    def _():
        row_down().start()

    @pl.when(has_high)
    def _():
        row_up().start()

    @pl.when(jnp.logical_not(has_low))
    def _():
        low_ref[...] = jnp.zeros_like(low_ref)

    @pl.when(jnp.logical_not(has_high))
    def _():
        high_ref[...] = jnp.zeros_like(high_ref)

    @pl.when(jnp.logical_not(has_low & is_last))
    def _():
        last_low_ref[...] = jnp.zeros_like(last_low_ref)

    @pl.when(jnp.logical_not(has_high & is_last))
    def _():
        last_high_ref[...] = jnp.zeros_like(last_high_ref)

    even = lax.rem(iota((levels, nlon), 1), TW)

    def field(r, carry):
        values = traj[r]
        top = values.astype(jnp.bfloat16).astype(jnp.float32)
        parts = [jnp.where(even == p, x, 0.0) for x in (top, values - top) for p in range(TW)]
        fields[r] = jnp.concatenate(parts, axis=0).T.astype(jnp.bfloat16)
        return carry

    lax.fori_loop(0, rows, field, 0)

    ids_land()
    ids = jnp.concatenate([ids_in[d] for d in range(count)], axis=0).astype(jnp.bfloat16)
    source = ones_where(iota((total, count), 0) // PAD == iota((total, count), 1)).astype(jnp.bfloat16)
    spread = dot(source, ids)
    nth = lax.rem(iota((total, LANES), 0), PAD)
    lanes = iota((total, LANES), 1)
    which = jnp.sum(jnp.where(lanes == nth, spread, 0.0), axis=1, keepdims=True)
    inner = jnp.sum(jnp.where(lanes == nth + PAD, spread, 0.0), axis=1, keepdims=True)
    which = jnp.broadcast_to(which, (total, LANES)).astype(jnp.bfloat16)
    pair = ones_where((lanes // TW).astype(jnp.float32) == inner).astype(jnp.bfloat16)
    nothing = jnp.zeros_like(pair)
    gathered = jnp.zeros((total, 2 * tile_len), jnp.float32)
    for r in range(rows):
        for c in range(columns):
            chosen[r, :, c * LANES : (c + 1) * LANES] = jnp.where(
                which == jnp.bfloat16(r * columns + c + 1), pair, nothing
            )
        gathered = gathered + dot(chosen[r], fields[r])
    states = gathered[:, :tile_len] + gathered[:, tile_len:]
    state_out[...] = states.reshape(count, PAD, tile_len)
    state_begin()

    loads[3].wait()

    def turn(k, carry):
        jac_t[k] = jac[k].astype(jnp.float32).T.astype(jnp.bfloat16)
        return carry

    lax.fori_loop(0, blocks, turn, 0, unroll=4)

    @pl.when(is_last)
    def _():
        def one(c, carry):
            span = pl.ds(pl.multiple_of(c * 16, 16), 16)

            def weigh(r):
                return coeff[r, span, :] * end[r, span, :].astype(jnp.float32)

            for r, near, ref in ((0, 1, edge_low), (rows - 1, rows - 2, edge_high)):
                mid = weigh(r)
                value = end[r, span, :].astype(jnp.float32) + weigh(near)
                value = value + pltpu.roll(mid, 1, 1) + pltpu.roll(mid, nlon - 1, 1) - 4.0 * mid
                ref[0, span, :] = mid.astype(jnp.bfloat16)
                ref[1, span, :] = (coeff[r, span, :] * value).astype(jnp.bfloat16)
            return carry

        lax.fori_loop(0, levels // 16, one, 0)

    @pl.when(has_low & is_last)
    def _():
        edge_down().start()

    @pl.when(has_high & is_last)
    def _():
        edge_up().start()

    order = iota((tile_len, tile_len), 0)
    other = iota((tile_len, tile_len), 1)

    def by_part(a, b):
        same = (a // TW == lax.rem(b, levels)) & (lax.rem(a, TW) == b // levels)
        return ones_where(same).astype(jnp.bfloat16)

    to_parts, from_parts = by_part(order, other), by_part(other, order)

    state_land()
    top, rest = split(state_in[...].reshape(total, tile_len))
    own = dot(place_t[...], jnp.concatenate([top, rest], axis=1)).astype(jnp.bfloat16)
    top, rest = dot(own[:, :tile_len], from_parts), dot(own[:, tile_len:], from_parts)
    groups = blocks // PAD
    for g in range(groups):
        span = slice(g * PAD, (g + 1) * PAD)
        state_rows[g] = jnp.concatenate([top[span], rest[span]], axis=0).astype(jnp.bfloat16)
    among = lax.rem(iota((2 * PAD, tile_len), 0), PAD)

    def product(both, mats, g):
        picked = jnp.zeros((2 * PAD, tile_len), jnp.float32)
        for i in range(PAD):
            picked = jnp.where(among == i, dot(both, mats[g * PAD + i]), picked)
        return picked[:PAD] + picked[PAD:]

    for g in range(groups):
        here = slice(g * PAD, (g + 1) * PAD)
        pred = product(state_rows[g], jac_t, g)
        weight = weight_ref[here, :] * valid_ref[here, :].astype(jnp.float32)
        resid = weight * (value_ref[here, :] - pred)
        top = resid.astype(jnp.bfloat16).astype(jnp.float32)
        resid_rows[g] = jnp.concatenate([top, resid - top], axis=0).astype(jnp.bfloat16)
    for g in range(groups):
        terms[g * PAD : (g + 1) * PAD, :] = product(resid_rows[g], jac, g)
    top, rest = split(terms[...])
    top, rest = dot(top, to_parts).astype(jnp.bfloat16), dot(rest, to_parts).astype(jnp.bfloat16)
    sent = dot(place[...], top) + dot(place[...], rest)
    term_out[...] = sent.reshape(count, PAD, tile_len)
    term_begin()
    ids_drain()
    state_drain()

    term_land()
    got = term_in[...].reshape(total, tile_len).T
    top, rest = split(got)
    parity = lax.rem(iota((levels, nlon), 1), TW)
    for r in range(rows):
        both = dot(top, chosen[r]) + dot(rest, chosen[r])
        forcing_ref[r] = jnp.where(parity == 0, both[:levels], both[levels:])
    term_drain()

    for cond, copy in (
        (has_low, row_down), (has_high, row_up), (has_low & is_last, edge_down), (has_high & is_last, edge_up)
    ):
        @pl.when(cond)
        def _(copy=copy):
            copy().wait_send()

    for cond, copy in (
        (has_high, row_down), (has_low, row_up), (has_high & is_last, edge_down), (has_low & is_last, edge_up)
    ):
        @pl.when(cond)
        def _(copy=copy):
            copy().wait_recv()


def observe(owner, tile, value, weight, valid, traj, coeff, end, jac, slots):
    lats = lax.axis_size("lat")
    count = lax.axis_size("tm") * lats
    _, rows, levels, nlon = traj.shape
    blocks = owner.shape[1]
    tile_len = levels * TW
    total = count * PAD
    bf16, f32 = jnp.bfloat16, jnp.float32
    edge = jax.ShapeDtypeStruct((SUB, levels, nlon), bf16)
    single = jax.ShapeDtypeStruct((1, levels, nlon), bf16)
    lists = pltpu.VMEM((count, 1, LANES), f32)
    parcels = pltpu.VMEM((count, PAD, tile_len), f32)
    stacked = pltpu.VMEM((blocks // PAD, 2 * PAD, tile_len), bf16)
    anywhere = pl.BlockSpec(memory_space=pl.ANY)
    dma = pltpu.SemaphoreType.DMA
    return pl.pallas_call(
        functools.partial(observe_kernel, lats, count, slots),
        out_shape=(jax.ShapeDtypeStruct((rows, levels, nlon), f32), single, single, edge, edge),
        in_specs=[VMEM] * 5 + [anywhere] * 4,
        out_specs=(VMEM,) * 5,
        scratch_shapes=[
            pltpu.VMEM((rows, levels, nlon), f32),
            pltpu.VMEM((rows, levels, nlon), f32),
            pltpu.VMEM((rows, levels, nlon), bf16),
            pltpu.VMEM(jac.shape, bf16),
            pltpu.VMEM(jac.shape, bf16),
            pltpu.VMEM((rows, nlon, 2 * tile_len), bf16),
            pltpu.VMEM((rows, total, nlon), bf16),
            pltpu.VMEM((total, blocks), bf16),
            pltpu.VMEM((blocks, total), bf16),
            lists, lists, parcels, parcels, parcels, parcels, stacked, stacked,
            pltpu.VMEM((blocks, tile_len), f32),
            pltpu.VMEM((1, levels, nlon), bf16),
            pltpu.VMEM((1, levels, nlon), bf16),
            pltpu.VMEM((SUB, levels, nlon), bf16),
            pltpu.VMEM((SUB, levels, nlon), bf16),
            dma((4,)),
        ]
        + [dma((count,))] * 6
        + [dma((2,))] * 4,
        compiler_params=pltpu.CompilerParams(
            collective_id=1, has_side_effects=True, vmem_limit_bytes=60 * 1024 * 1024
        ),
        name="observe",
    )(owner, tile, value, weight, valid, traj, coeff, end, jac)


def chain_kernel(
    sections, lats, coeff_ref, low_ref, high_ref, last_low_ref, last_high_ref, end_ref, forcing_ref, out_ref,
    main, low, high, edge_low, edge_high, ahead, weighted, partial, second,
    main_send, main_recv, down_send, up_send, low_recv, high_recv,
):
    section, band = lax.axis_index("tm"), lax.axis_index("lat")
    rows, levels, nlon = end_ref.shape
    chunks = levels // CHUNK
    is_last = section == sections - 1
    has_before, has_low, has_high = section > 0, band > 0, band < lats - 1

    sends_low, sends_high = has_low & jnp.logical_not(is_last), has_high & jnp.logical_not(is_last)

    barrier = pltpu.get_barrier_semaphore()
    sides = (
        (jnp.logical_not(is_last), section + 1, band),
        (has_before, section - 1, band),
        (has_low, section, band - 1),
        (has_high, section, band + 1),
    )
    for there, tm, lat in sides:
        @pl.when(there)
        def _(tm=tm, lat=lat):
            pl.semaphore_signal(barrier, inc=1, device_id=(tm, lat), device_id_type=MESH)
    pl.semaphore_wait(barrier, sum(there.astype(jnp.int32) for there, _, _ in sides))

    def remote(src, dst, send, recv, tm, lat):
        return pltpu.make_async_remote_copy(
            src_ref=src, dst_ref=dst, send_sem=send, recv_sem=recv, device_id=(tm, lat), device_id_type=MESH
        )

    def local_main(c):
        return pltpu.make_async_copy(
            end_ref.at[:, pl.ds(pl.multiple_of(c * CHUNK, CHUNK), CHUNK), :], main.at[c], main_recv.at[c]
        )

    def handed(c):
        return remote(ahead.at[c], main.at[c], main_send.at[c], main_recv.at[c], section - 1, band)

    def downward(c):
        return remote(edge_low.at[c], high.at[c], down_send.at[c], high_recv.at[c], section, band - 1)

    def upward(c):
        return remote(edge_high.at[c], low.at[c], up_send.at[c], low_recv.at[c], section, band + 1)

    @pl.when(jnp.logical_not(has_low))
    def _():
        low[...] = jnp.zeros_like(low)

    @pl.when(jnp.logical_not(has_high))
    def _():
        high[...] = jnp.zeros_like(high)

    @pl.when(is_last)
    def _():
        for c in range(chunks):
            local_main(c).start()
            low[c] = last_low_ref[:, c * CHUNK : (c + 1) * CHUNK, :]
            high[c] = last_high_ref[:, c * CHUNK : (c + 1) * CHUNK, :]

    def levels_of(c):
        return pl.ds(pl.multiple_of(c * CHUNK, CHUNK), CHUNK)

    def along(mid):
        return pltpu.roll(mid, 1, 1) + pltpu.roll(mid, nlon - 1, 1) - 4.0 * mid

    def begin(c):
        @pl.when(is_last)
        def _():
            local_main(c).wait()

        @pl.when(jnp.logical_not(is_last))
        def _():
            handed(c).wait_recv()

        span = levels_of(c)
        for r in range(rows):
            weighted[c, r] = coeff_ref[0, r, span, :] * main[c, r].astype(jnp.float32)
        for r in range(rows):
            mid = weighted[c, r]
            value = main[c, r].astype(jnp.float32) + along(mid)
            if r > 0:
                value = value + weighted[c, r - 1]
            if r < rows - 1:
                value = value + weighted[c, r + 1]
            partial[c, r] = value
            if r == 0:
                edge_low[c, 0] = mid.astype(jnp.bfloat16)
                edge_low[c, 1] = (coeff_ref[0, r, span, :] * value).astype(jnp.bfloat16)
            if r == rows - 1:
                edge_high[c, 0] = mid.astype(jnp.bfloat16)
                edge_high[c, 1] = (coeff_ref[0, r, span, :] * value).astype(jnp.bfloat16)

        @pl.when(sends_low)
        def _():
            downward(c).start()

        @pl.when(sends_high)
        def _():
            upward(c).start()

    def complete(c):
        span = levels_of(c)
        end = rows - 1
        partial[c, 0] = partial[c, 0] + low[c, 0].astype(jnp.float32)
        partial[c, end] = partial[c, end] + high[c, 0].astype(jnp.float32)
        second[0] = low[c, 1].astype(jnp.float32) + low_ref[0, span, :].astype(jnp.float32) * weighted[c, 0]
        second[rows + 1] = high[c, 1].astype(jnp.float32) + high_ref[0, span, :].astype(jnp.float32) * weighted[c, end]
        for r in range(rows):
            second[r + 1] = coeff_ref[0, r, span, :] * partial[c, r]
        for r in range(rows):
            value = partial[c, r] + second[r] + second[r + 2] + along(second[r + 1]) + forcing_ref[r, span, :]
            out_ref[0, r, span, :] = value
            ahead[c, r] = value.astype(jnp.bfloat16)

    look = jnp.where(section == sections - 2, min(4, chunks), min(2, chunks))

    def open_one(c, carry):
        begin(c)
        return carry

    lax.fori_loop(0, look, open_one, 0)

    def step(c, carry):
        @pl.when(c + look < chunks)
        def _():
            begin(c + look)

        @pl.when(sends_low)
        def _():
            upward(c).wait_recv()

        @pl.when(sends_high)
        def _():
            downward(c).wait_recv()

        complete(c)

        @pl.when(has_before)
        def _():
            handed(c).start()

        return carry

    lax.fori_loop(0, chunks, step, 0)

    def finish(c, carry):
        @pl.when(sends_low)
        def _():
            downward(c).wait_send()

        @pl.when(sends_high)
        def _():
            upward(c).wait_send()

        @pl.when(has_before)
        def _():
            handed(c).wait_send()

        return carry

    lax.fori_loop(0, chunks, finish, 0)


def chain(coeff, low, high, last_low, last_high, end, forcing):
    rows, levels, nlon = end.shape
    chunks = levels // CHUNK
    part = lambda n, kind: pltpu.VMEM((chunks, n, CHUNK, nlon), kind)
    return pl.pallas_call(
        functools.partial(chain_kernel, lax.axis_size("tm"), lax.axis_size("lat")),
        out_shape=jax.ShapeDtypeStruct(coeff.shape, jnp.float32),
        in_specs=[VMEM] * 7,
        out_specs=VMEM,
        scratch_shapes=[
            part(rows, jnp.bfloat16),
            part(SUB, jnp.bfloat16),
            part(SUB, jnp.bfloat16),
            part(SUB, jnp.bfloat16),
            part(SUB, jnp.bfloat16),
            part(rows, jnp.bfloat16),
            part(rows, jnp.float32),
            part(rows, jnp.float32),
            pltpu.VMEM((rows + 2, CHUNK, nlon), jnp.float32),
        ]
        + [pltpu.SemaphoreType.DMA((chunks,))] * 6,
        compiler_params=pltpu.CompilerParams(
            collective_id=9, has_side_effects=True, vmem_limit_bytes=48 * 1024 * 1024
        ),
        name="chain",
    )(coeff, low, high, last_low, last_high, end, forcing)


def per_device(
    trajectory,
    diffusivity,
    adjoint_end,
    obs_jac,
    obs_value,
    obs_weight,
    obs_valid,
    obs_owner,
    obs_tile,
):
    devices = lax.axis_size("tm") * lax.axis_size("lat")
    blocks = obs_owner.shape[0]
    slots = max(2, 2 * blocks // devices)
    forcing, low, high, last_low, last_high = observe(
        obs_owner[:, 0][None, :], obs_tile[None, :], obs_value, obs_weight, obs_valid,
        trajectory, diffusivity, adjoint_end, obs_jac, slots,
    )
    return chain(diffusivity, low, high, last_low, last_high, adjoint_end, forcing)


def solution(mesh):
    in_specs = (
        P("tm", "lat", None, None),
        P("tm", "lat", None, None),
        P("lat", None, None),
        P(("tm", "lat"), None, None),
        P(("tm", "lat"), None),
        P(("tm", "lat"), None),
        P(("tm", "lat"), None),
        P(("tm", "lat"), None),
        P(("tm", "lat")),
    )
    out_specs = P("tm", "lat", None, None)
    return jax.shard_map(
        per_device, mesh=mesh, in_specs=in_specs, out_specs=out_specs, check_vma=False
    )
```

```python
import functools

import jax
import jax.numpy as jnp
from jax import lax
from jax.experimental import pallas as pl
from jax.experimental.pallas import tpu as pltpu
from jax.sharding import PartitionSpec as P

TW = 2
SUB = 2
LANES = 128
PAD = 8
CHUNK = 8
SCALE = 2.0**17
MESH = pl.DeviceIdType.MESH
VMEM = pl.BlockSpec(memory_space=pltpu.VMEM)


def split(x):
    top = x.astype(jnp.bfloat16)
    return top, (x - top.astype(jnp.float32)).astype(jnp.bfloat16)


def dot(a, b):
    return jnp.dot(a, b, preferred_element_type=jnp.float32)


def iota(shape, axis):
    return lax.broadcasted_iota(jnp.int32, shape, axis)


def ones_where(mask):
    return jnp.where(mask, 1.0, 0.0)


def sweep_kernel(
    lats, sections, slots,
    owner_hbm, tile_hbm, value_hbm, weight_hbm, valid_hbm, traj_hbm, coeff_hbm, end_hbm, jac_hbm,
    out_ref,
    owner_ref, tile_ref, value_ref, weight_ref, valid_ref, traj, coeff, jac, jac_t, fields, chosen, place, place_t, which, pair,
    ids_out, ids_in, state_out, state_in, term_out, term_in, state_rows, resid_rows, terms, terms_t,
    coded, kappa, kappa_low, kappa_high, main, forcing, weighted, partial, second, early,
    edge_low, edge_high, low, high,
    load_sem, end_sem, ids_send, ids_recv, state_send, state_recv, term_send, term_recv,
    kappa_send, kappa_recv, down_send, down_recv, up_send, up_recv,
    low_send, low_recv, high_send, high_recv, out_send, out_recv,
):
    section, band = lax.axis_index("tm"), lax.axis_index("lat")
    count = sections * lats
    me = section * lats + band
    rows, levels, nlon = coeff.shape
    blocks = owner_ref.shape[1]
    total = count * PAD
    columns = nlon // LANES
    per_column = LANES // TW
    tile_len = levels * TW
    part = levels // sections
    chunks = part // CHUNK
    width = part * TW
    has_low, has_high = band > 0, band < lats - 1
    last = sections - 1

    loads = [
        pltpu.make_async_copy(src, dst, load_sem.at[i])
        for i, (src, dst) in enumerate(
            (
                (owner_hbm, owner_ref), (tile_hbm, tile_ref), (coeff_hbm.at[0], coeff), (traj_hbm.at[0], traj),
                (jac_hbm, jac), (value_hbm, value_ref), (weight_hbm, weight_ref), (valid_hbm, valid_ref),
            )
        )
    ]
    for load in loads:
        load.start()

    def end_load(c):
        at = pl.multiple_of(section * part + c * CHUNK, CHUNK)
        return pltpu.make_async_copy(end_hbm.at[:, pl.ds(at, CHUNK), :], main.at[sections, c], end_sem.at[c])

    for c in range(chunks):
        end_load(c).start()

    barrier = pltpu.get_barrier_semaphore()

    def peer(j):
        to = lax.rem(me + j, count)
        return to, (to // lats, lax.rem(to, lats))

    def greet(j, carry):
        pl.semaphore_signal(barrier, inc=1, device_id=peer(j)[1], device_id_type=MESH)
        return carry

    lax.fori_loop(1, count, greet, 0)

    def remote(src, dst, send, recv, where):
        return pltpu.make_async_remote_copy(
            src_ref=src, dst_ref=dst, send_sem=send, recv_sem=recv, device_id=where, device_id_type=MESH
        )

    def swap(pick, into, send, recv):
        def outgoing(j):
            to, where = peer(j)
            return remote(pick(to), into.at[me], send.at[j], recv.at[j], where)

        def incoming(j):
            source, where = peer(count - j)
            return remote(pick(source), into.at[source], send.at[j], recv.at[j], where)

        def launch(j, carry):
            outgoing(j).start()
            return carry

        def land(j, carry):
            incoming(j).wait_recv()
            return carry

        def drain(j, carry):
            outgoing(j).wait_send()
            return carry

        def begin():
            lax.fori_loop(1, count, launch, 0)
            into[me] = pick(me)[...]

        return begin, lambda: lax.fori_loop(1, count, land, 0), lambda: lax.fori_loop(1, count, drain, 0)

    ids_begin, ids_land, ids_drain = swap(lambda d: ids_out.at[lax.rem(d, lats)], ids_in, ids_send, ids_recv)
    state_begin, state_land, state_drain = swap(lambda d: state_out.at[d], state_in, state_send, state_recv)
    term_begin, term_land, term_drain = swap(lambda d: term_out.at[d], term_in, term_send, term_recv)

    for load in loads[:2]:
        load.wait()
    owner = owner_ref[...]
    mine = owner == iota((count, blocks), 0)
    before = ones_where(iota((blocks, blocks), 0) < iota((blocks, blocks), 1)).astype(jnp.bfloat16)
    rank = dot(ones_where(mine).astype(jnp.bfloat16), before)
    target = jnp.where(mine, iota((count, blocks), 0).astype(jnp.float32) * PAD + rank, 0.0)
    slot = jnp.sum(target, axis=0, keepdims=True)
    tile = tile_ref[...]
    column = (tile // per_column + 1).astype(jnp.float32)
    inside = lax.rem(tile, per_column).astype(jnp.float32)
    lane = iota((count, LANES), 1)
    packed = jnp.zeros((count, LANES), jnp.float32)
    for s in range(slots):
        here = mine & (rank == float(s))
        for at, what in ((s, column), (PAD + s, inside)):
            found = jnp.sum(jnp.where(here, what, 0.0), axis=1, keepdims=True)
            packed = jnp.where(lane == at, found, packed)
    lists = packed[:lats]
    for s in range(1, sections):
        lists = lists + pltpu.roll(packed[s * lats : (s + 1) * lats], s * 2 * PAD, 1)
    for b in range(lats):
        ids_out[b] = lists[b : b + 1]
    pl.semaphore_wait(barrier, count - 1)
    ids_begin()

    def kappa_copy(j):
        to = lax.rem(section + j, sections)
        return remote(coded.at[to], kappa.at[section], kappa_send.at[j], kappa_recv.at[j], (to, band))

    def kappa_arrival(j):
        source = lax.rem(section + sections - j, sections)
        return remote(coded.at[source], kappa.at[source], kappa_send.at[j], kappa_recv.at[j], (source, band))

    def row_down(j):
        to = lax.rem(section + j, sections)
        return remote(coded.at[to, :, 0], kappa_high.at[section], down_send.at[j], down_recv.at[j], (to, band - 1))

    def row_up(j):
        to = lax.rem(section + j, sections)
        return remote(coded.at[to, :, rows - 1], kappa_low.at[section], up_send.at[j], up_recv.at[j], (to, band + 1))

    def from_high(j):
        source = lax.rem(section + sections - j, sections)
        return remote(coded.at[source, :, 0], kappa_high.at[source], down_send.at[j], down_recv.at[j], (source, band))

    def from_low(j):
        source = lax.rem(section + sections - j, sections)
        return remote(coded.at[source, :, 0], kappa_low.at[source], up_send.at[j], up_recv.at[j], (source, band))

    def share():
        for j in range(1, sections):
            kappa_copy(j).start()

        @pl.when(has_low)
        def _():
            for j in range(sections):
                row_down(j).start()

        @pl.when(has_high)
        def _():
            for j in range(sections):
                row_up(j).start()

    loads[2].wait()

    def encode(q, carry):
        for c in range(chunks):
            at = pl.multiple_of(q * part + c * CHUNK, CHUNK)
            for r in range(rows):
                scaled = coeff[r, pl.ds(at, CHUNK), :] * SCALE + 0.5
                coded[q, c, r] = scaled.astype(jnp.int32).astype(jnp.int16)
        return carry

    lax.fori_loop(0, sections, encode, 0)
    is_odd = lax.rem(section, 2) == lax.rem(last, 2)

    @pl.when(is_odd)
    def _():
        share()

    kappa[section] = coded[section]

    holds = ones_where(iota((total, blocks), 0).astype(jnp.float32) == slot)
    place[...] = holds.astype(jnp.bfloat16)
    place_t[...] = holds.T.astype(jnp.bfloat16)

    @pl.when(jnp.logical_not(has_low))
    def _():
        low[...] = jnp.zeros_like(low)
        kappa_low[...] = jnp.zeros_like(kappa_low)

    @pl.when(jnp.logical_not(has_high))
    def _():
        high[...] = jnp.zeros_like(high)
        kappa_high[...] = jnp.zeros_like(kappa_high)

    loads[3].wait()
    even = lax.rem(iota((levels, nlon), 1), TW)

    def field(r, carry):
        values = traj[r]
        top = values.astype(jnp.bfloat16).astype(jnp.float32)
        parts = [jnp.where(even == p, x, 0.0) for x in (top, values - top) for p in range(TW)]
        fields[r] = jnp.concatenate(parts, axis=0).T.astype(jnp.bfloat16)
        return carry

    lax.fori_loop(0, rows, field, 0)

    ids_land()
    ids = jnp.concatenate([ids_in[d] for d in range(count)], axis=0).astype(jnp.bfloat16)
    source = ones_where(iota((total, count), 0) // PAD == iota((total, count), 1)).astype(jnp.bfloat16)
    spread = dot(source, ids)
    nth = lax.rem(iota((total, LANES), 0), PAD)
    lanes = iota((total, LANES), 1)

    def listed(s):
        at = nth + s * 2 * PAD
        outer = jnp.sum(jnp.where(lanes == at, spread, 0.0), axis=1, keepdims=True)
        inner = jnp.sum(jnp.where(lanes == at + PAD, spread, 0.0), axis=1, keepdims=True)
        which[s] = jnp.broadcast_to(outer, (total, LANES)).astype(jnp.bfloat16)
        pair[s] = ones_where((lanes // TW).astype(jnp.float32) == inner).astype(jnp.bfloat16)

    nothing = jnp.zeros((total, LANES), jnp.bfloat16)

    def tiles(s, r, c):
        return jnp.where(which[s] == jnp.bfloat16(r * columns + c + 1), pair[s], nothing)

    listed(section)
    gathered = jnp.zeros((total, 2 * tile_len), jnp.float32)
    for r in range(rows):
        for c in range(columns):
            chosen[r, :, c * LANES : (c + 1) * LANES] = tiles(section, r, c)
        gathered = gathered + dot(chosen[r], fields[r])
    states = gathered[:, :tile_len] + gathered[:, tile_len:]
    state_out[...] = states.reshape(count, PAD, tile_len)
    state_begin()

    @pl.when(jnp.logical_not(is_odd))
    def _():
        share()

    for load in loads[4:]:
        load.wait()

    def turn(k, carry):
        jac_t[k] = jac[k].astype(jnp.float32).T.astype(jnp.bfloat16)
        return carry

    lax.fori_loop(0, blocks, turn, 0, unroll=4)

    def list_other(j, carry):
        listed(lax.rem(section + j, sections))
        return carry

    lax.fori_loop(1, sections, list_other, 0)

    def downward(s, c):
        return remote(edge_low.at[s, c], high.at[s, c], low_send.at[s, c], high_recv.at[s, c], (section, band - 1))

    def upward(s, c):
        return remote(edge_high.at[s, c], low.at[s, c], high_send.at[s, c], low_recv.at[s, c], (section, band + 1))

    def along(mid):
        return pltpu.roll(mid, 1, 1) + pltpu.roll(mid, nlon - 1, 1) - 4.0 * mid

    def decode(x):
        return x.astype(jnp.int32).astype(jnp.float32) * (1.0 / SCALE)

    def begin(s, c):
        for r in range(rows):
            weighted[c, r] = decode(kappa[s, c, r]) * main[s + 1, c, r].astype(jnp.float32)
        for r in range(rows):
            mid = weighted[c, r]
            value = main[s + 1, c, r].astype(jnp.float32) + along(mid)
            if r > 0:
                value = value + weighted[c, r - 1]
            if r < rows - 1:
                value = value + weighted[c, r + 1]
            partial[c, r] = value
            for at, ref in ((0, edge_low), (rows - 1, edge_high)):
                if r == at:
                    ref[s, c, 0] = mid.astype(jnp.bfloat16)
                    ref[s, c, 1] = (decode(kappa[s, c, r]) * value).astype(jnp.bfloat16)

        @pl.when(has_low)
        def _():
            downward(s, c).start()

        @pl.when(has_high)
        def _():
            upward(s, c).start()

    def complete(s, c, store):
        @pl.when(has_low)
        def _():
            upward(s, c).wait_recv()

        @pl.when(has_high)
        def _():
            downward(s, c).wait_recv()

        end = rows - 1
        partial[c, 0] = partial[c, 0] + low[s, c, 0].astype(jnp.float32)
        partial[c, end] = partial[c, end] + high[s, c, 0].astype(jnp.float32)
        second[0] = low[s, c, 1].astype(jnp.float32) + decode(kappa_low[s, c]) * weighted[c, 0]
        second[rows + 1] = high[s, c, 1].astype(jnp.float32) + decode(kappa_high[s, c]) * weighted[c, end]
        for r in range(rows):
            second[r + 1] = decode(kappa[s, c, r]) * partial[c, r]
        for r in range(rows):
            store(r, partial[c, r] + second[r] + second[r + 2] + along(second[r + 1]))

    def spot(q, c):
        return out_ref.at[:, pl.ds(pl.multiple_of(q * part + c * CHUNK, CHUNK), CHUNK), :]

    def give(s, c):
        return remote(main.at[s, c], spot(section, c), out_send.at[s, c], out_recv.at[section, c], (s, band))

    def taken(q, c):
        return remote(main.at[q, c], spot(q, c), out_send.at[q, c], out_recv.at[q, c], (q, band))

    def finish(s, c, r, value):
        main[s, c, r] = value.astype(jnp.bfloat16)

    def deliver(s, c):
        @pl.when(s != section)
        def _():
            give(s, c).start()

        @pl.when(s == section)
        def _():
            spot(section, c)[...] = main[s, c]

    last_from = lax.rem(section + 1, sections)

    @pl.when(last_from != 0)
    def _():
        kappa_arrival(last_from).wait_recv()

    for c in range(chunks):
        end_load(c).wait()

    def open_last(c, carry):
        begin(last, c)
        return carry

    lax.fori_loop(0, chunks, open_last, 0)

    order = iota((tile_len, tile_len), 0)
    other = iota((tile_len, tile_len), 1)

    def by_part(a, b, size):
        level = a // TW
        place_of = (level // size) * (size * TW) + lax.rem(a, TW) * size + lax.rem(level, size)
        return ones_where(place_of == b).astype(jnp.bfloat16)

    to_parts, from_parts = by_part(order, other, part), by_part(other, order, levels)

    state_land()
    top, rest = split(state_in[...].reshape(total, tile_len))
    own = dot(place_t[...], jnp.concatenate([top, rest], axis=1)).astype(jnp.bfloat16)
    top, rest = dot(own[:, :tile_len], from_parts), dot(own[:, tile_len:], from_parts)
    groups = blocks // PAD
    for g in range(groups):
        span = slice(g * PAD, (g + 1) * PAD)
        state_rows[g] = jnp.concatenate([top[span], rest[span]], axis=0).astype(jnp.bfloat16)
    among = lax.rem(iota((2 * PAD, tile_len), 0), PAD)

    def product(both, mats, g):
        picked = jnp.zeros((2 * PAD, tile_len), jnp.float32)
        for i in range(PAD):
            picked = jnp.where(among == i, dot(both, mats[g * PAD + i]), picked)
        return picked[:PAD] + picked[PAD:]

    for g in range(groups):
        here = slice(g * PAD, (g + 1) * PAD)
        pred = product(state_rows[g], jac_t, g)
        weight = weight_ref[here, :] * valid_ref[here, :].astype(jnp.float32)
        resid = weight * (value_ref[here, :] - pred)
        top = resid.astype(jnp.bfloat16).astype(jnp.float32)
        resid_rows[g] = jnp.concatenate([top, resid - top], axis=0).astype(jnp.bfloat16)
    for g in range(groups):
        terms[g * PAD : (g + 1) * PAD, :] = product(resid_rows[g], jac, g)
    top, rest = split(terms[...])
    top, rest = dot(top, to_parts).astype(jnp.bfloat16), dot(rest, to_parts).astype(jnp.bfloat16)
    sent = dot(place[...], top) + dot(place[...], rest)
    group = lats * PAD
    strip = iota((group, tile_len), 1) // width
    for q in range(sections):
        parcel = jnp.zeros((group, tile_len), jnp.float32)
        for s in range(sections):
            moved = sent[s * group : (s + 1) * group]
            if s != q:
                moved = pltpu.roll(moved, ((s - q) % sections) * width, 1)
            parcel = jnp.where(strip == s, moved, parcel)
        term_out[q * lats : (q + 1) * lats] = parcel.reshape(lats, PAD, tile_len)
    term_begin()
    ids_drain()
    state_drain()

    for j in range(sections):
        @pl.when(has_high)
        def _(j=j):
            from_high(j).wait_recv()

        @pl.when(has_low)
        def _(j=j):
            from_low(j).wait_recv()

    def kappa_land(j, carry):
        @pl.when(j != last_from)
        def _():
            kappa_arrival(j).wait_recv()

        return carry

    lax.fori_loop(1, sections, kappa_land, 0)

    def close_last(c, carry):
        def keep(r, value):
            early[c, r] = value

        complete(last, c, keep)
        return carry

    lax.fori_loop(0, chunks, close_last, 0)

    term_land()
    got = term_in[...].reshape(total, tile_len).T
    top = got.astype(jnp.bfloat16).astype(jnp.float32)
    rest = got - top
    for s in range(sections):
        span = slice(s * width, (s + 1) * width)
        stack = jnp.concatenate([top[span], rest[span]], axis=0).astype(jnp.bfloat16)
        terms_t[s] = stack
    wide = 2 * LANES
    parity = lax.rem(iota((part, wide), 1), TW)

    def scatter(s):
        left = terms_t[s]
        for r in range(rows):
            for c in range(nlon // wide):
                right = jnp.concatenate([tiles(s, r, 2 * c), tiles(s, r, 2 * c + 1)], axis=1)
                both = dot(left, right)
                both = both[:width] + both[width:]
                value = jnp.where(parity == 0, both[:part], both[part:])
                for k in range(chunks):
                    forcing[s, k, r, :, c * wide : (c + 1) * wide] = value[k * CHUNK : (k + 1) * CHUNK]

    scatter(last)

    def start_last(c, carry):
        for r in range(rows):
            finish(last, c, r, early[c, r] + forcing[last, c, r])
        if last > 0:
            begin(last - 1, c)
        deliver(last, c)
        return carry

    lax.fori_loop(0, chunks, start_last, 0)

    def scatter_other(j, carry):
        scatter(last - j)
        return carry

    lax.fori_loop(1, sections, scatter_other, 0)

    def go(i, carry):
        s = last - 1 - i // chunks
        c = lax.rem(i, chunks)
        complete(s, c, lambda r, value: finish(s, c, r, value + forcing[s, c, r]))

        @pl.when(s > 0)
        def _():
            begin(s - 1, c)

        deliver(s, c)
        return carry

    lax.fori_loop(0, last * chunks, go, 0)

    term_drain()
    for j in range(1, sections):
        kappa_copy(j).wait_send()
    for cond, copy in ((has_low, row_down), (has_high, row_up)):
        @pl.when(cond)
        def _(copy=copy):
            for j in range(sections):
                copy(j).wait_send()

    def settle(i, carry):
        s, c = i // chunks, lax.rem(i, chunks)

        @pl.when(has_low)
        def _():
            downward(s, c).wait_send()

        @pl.when(has_high)
        def _():
            upward(s, c).wait_send()

        @pl.when(s != section)
        def _():
            give(s, c).wait_send()

        return carry

    lax.fori_loop(0, sections * chunks, settle, 0)

    def gain(i, carry):
        q, c = lax.rem(section + 1 + i // chunks, sections), lax.rem(i, chunks)
        taken(q, c).wait_recv()
        return carry

    lax.fori_loop(0, last * chunks, gain, 0)


def sweep(owner, tile, value, weight, valid, traj, coeff, end, jac, slots):
    lats, sections = lax.axis_size("lat"), lax.axis_size("tm")
    count = sections * lats
    _, rows, levels, nlon = traj.shape
    blocks = owner.shape[1]
    tile_len = levels * TW
    total = count * PAD
    chunks = levels // sections // CHUNK
    bf16, f32 = jnp.bfloat16, jnp.float32
    parcels = pltpu.VMEM((count, PAD, tile_len), f32)
    stacked = pltpu.VMEM((blocks // PAD, 2 * PAD, tile_len), bf16)
    work = pltpu.VMEM((chunks, rows, CHUNK, nlon), f32)
    edges = pltpu.VMEM((sections, chunks, SUB, CHUNK, nlon), bf16)
    codes = lambda *lead: pltpu.VMEM(lead + (CHUNK, nlon), jnp.int16)
    hbm = pl.BlockSpec(memory_space=pltpu.HBM)
    dma = pltpu.SemaphoreType.DMA
    return pl.pallas_call(
        functools.partial(sweep_kernel, lats, sections, slots),
        out_shape=jax.ShapeDtypeStruct((rows, levels, nlon), bf16),
        in_specs=[hbm] * 9,
        out_specs=VMEM,
        scratch_shapes=[
            pltpu.VMEM(owner.shape, owner.dtype),
            pltpu.VMEM(tile.shape, tile.dtype),
            pltpu.VMEM(value.shape, value.dtype),
            pltpu.VMEM(weight.shape, weight.dtype),
            pltpu.VMEM(valid.shape, valid.dtype),
            pltpu.VMEM((rows, levels, nlon), f32),
            pltpu.VMEM((rows, levels, nlon), f32),
            pltpu.VMEM(jac.shape, bf16),
            pltpu.VMEM(jac.shape, bf16),
            pltpu.VMEM((rows, nlon, 2 * tile_len), bf16),
            pltpu.VMEM((rows, total, nlon), bf16),
            pltpu.VMEM((total, blocks), bf16),
            pltpu.VMEM((blocks, total), bf16),
            pltpu.VMEM((sections, total, LANES), bf16),
            pltpu.VMEM((sections, total, LANES), bf16),
            pltpu.VMEM((lats, 1, LANES), f32),
            pltpu.VMEM((count, 1, LANES), f32),
            parcels, parcels, parcels, parcels, stacked, stacked,
            pltpu.VMEM((blocks, tile_len), f32),
            pltpu.VMEM((sections, 2 * tile_len // sections, total), bf16),
            codes(sections, chunks, rows),
            codes(sections, chunks, rows),
            codes(sections, chunks),
            codes(sections, chunks),
            pltpu.VMEM((sections + 1, chunks, rows, CHUNK, nlon), bf16),
            pltpu.VMEM((sections, chunks, rows, CHUNK, nlon), f32),
            work, work,
            pltpu.VMEM((rows + 2, CHUNK, nlon), f32),
            work,
            edges, edges, edges, edges,
            dma((8,)),
            dma((chunks,)),
        ]
        + [dma((count,))] * 6
        + [dma((sections,))] * 6
        + [dma((sections, chunks))] * 6,
        compiler_params=pltpu.CompilerParams(
            collective_id=1, has_side_effects=True, vmem_limit_bytes=63 * 1024 * 1024
        ),
        name="sweep",
    )(owner, tile, value, weight, valid, traj, coeff, end, jac)


def per_device(
    trajectory,
    diffusivity,
    adjoint_end,
    obs_jac,
    obs_value,
    obs_weight,
    obs_valid,
    obs_owner,
    obs_tile,
):
    devices = lax.axis_size("tm") * lax.axis_size("lat")
    blocks = obs_owner.shape[0]
    slots = max(2, 2 * blocks // devices)
    rounded = sweep(
        obs_owner[:, 0][None, :], obs_tile[None, :], obs_value, obs_weight, obs_valid,
        trajectory, diffusivity, adjoint_end, obs_jac, slots,
    )
    return rounded.astype(jnp.float32)[None]


def solution(mesh):
    in_specs = (
        P("tm", "lat", None, None),
        P("tm", "lat", None, None),
        P("lat", None, None),
        P(("tm", "lat"), None, None),
        P(("tm", "lat"), None),
        P(("tm", "lat"), None),
        P(("tm", "lat"), None),
        P(("tm", "lat"), None),
        P(("tm", "lat")),
    )
    out_specs = P("tm", "lat", None, None)
    return jax.shard_map(
        per_device, mesh=mesh, in_specs=in_specs, out_specs=out_specs, check_vma=False
    )
```

```python
import functools

import jax
import jax.numpy as jnp
from jax import lax
from jax.experimental import pallas as pl
from jax.experimental.pallas import tpu as pltpu
from jax.sharding import PartitionSpec as P

TW = 2
SUB = 2
LANES = 128
PAD = 8
CHUNK = 8
SCALE = 2.0**17
MESH = pl.DeviceIdType.MESH
VMEM = pl.BlockSpec(memory_space=pltpu.VMEM)


def split(x):
    top = x.astype(jnp.bfloat16)
    return top, (x - top.astype(jnp.float32)).astype(jnp.bfloat16)


def dot(a, b):
    return jnp.dot(a, b, preferred_element_type=jnp.float32)


def iota(shape, axis):
    return lax.broadcasted_iota(jnp.int32, shape, axis)


def ones_where(mask):
    return jnp.where(mask, 1.0, 0.0)


def sweep_kernel(
    lats, sections, slots,
    owner_hbm, tile_hbm, value_hbm, weight_hbm, valid_hbm, traj_hbm, coeff_hbm, end_hbm, jac_hbm,
    out_ref,
    owner_ref, tile_ref, value_ref, weight_ref, valid_ref, traj, coeff, jac, jac_t, fields, chosen, place, place_t, which, pair,
    ids_out, ids_in, state_out, state_in, term_out, term_in, state_rows, resid_rows, terms, terms_t,
    coded, kappa, kappa_low, kappa_high, main, forcing, weighted, partial, second, early,
    edge_low, edge_high, low, high,
    load_sem, end_sem, ids_send, ids_recv, state_send, state_recv, term_send, term_recv,
    kappa_send, kappa_recv, down_send, down_recv, up_send, up_recv,
    low_send, low_recv, high_send, high_recv, out_send, out_recv, own_sem,
):
    section, band = lax.axis_index("tm"), lax.axis_index("lat")
    count = sections * lats
    me = section * lats + band
    rows, levels, nlon = coeff.shape
    blocks = owner_ref.shape[1]
    total = count * PAD
    columns = nlon // LANES
    per_column = LANES // TW
    tile_len = levels * TW
    part = levels // sections
    chunks = part // CHUNK
    width = part * TW
    has_low, has_high = band > 0, band < lats - 1
    last = sections - 1

    loads = [
        pltpu.make_async_copy(src, dst, load_sem.at[i])
        for i, (src, dst) in enumerate(
            (
                (owner_hbm, owner_ref), (tile_hbm, tile_ref), (coeff_hbm.at[0], coeff), (traj_hbm.at[0], traj),
                (jac_hbm, jac), (value_hbm, value_ref), (weight_hbm, weight_ref), (valid_hbm, valid_ref),
            )
        )
    ]
    for load in loads:
        load.start()

    def end_load(c):
        at = pl.multiple_of(section * part + c * CHUNK, CHUNK)
        return pltpu.make_async_copy(end_hbm.at[:, pl.ds(at, CHUNK), :], main.at[sections, c], end_sem.at[c])

    for c in range(chunks):
        end_load(c).start()

    barrier = pltpu.get_barrier_semaphore()

    def peer(j):
        to = lax.rem(me + j, count)
        return to, (to // lats, lax.rem(to, lats))

    def greet(j, carry):
        pl.semaphore_signal(barrier, inc=1, device_id=peer(j)[1], device_id_type=MESH)
        return carry

    lax.fori_loop(1, count, greet, 0)

    def remote(src, dst, send, recv, where):
        return pltpu.make_async_remote_copy(
            src_ref=src, dst_ref=dst, send_sem=send, recv_sem=recv, device_id=where, device_id_type=MESH
        )

    def swap(pick, into, send, recv, used):
        def outgoing(j):
            to, where = peer(j)
            return remote(pick(to).at[:used], into.at[me, :used], send.at[j], recv.at[j], where)

        def incoming(j):
            source, where = peer(count - j)
            return remote(pick(source).at[:used], into.at[source, :used], send.at[j], recv.at[j], where)

        def launch(j, carry):
            outgoing(j).start()
            return carry

        def land(j, carry):
            incoming(j).wait_recv()
            return carry

        def drain(j, carry):
            outgoing(j).wait_send()
            return carry

        def begin():
            lax.fori_loop(1, count, launch, 0)
            into[me] = pick(me)[...]

        return begin, lambda: lax.fori_loop(1, count, land, 0), lambda: lax.fori_loop(1, count, drain, 0)

    ids_begin, ids_land, ids_drain = swap(lambda d: ids_out.at[lax.rem(d, lats)], ids_in, ids_send, ids_recv, 1)
    state_begin, state_land, state_drain = swap(lambda d: state_out.at[d], state_in, state_send, state_recv, slots)
    term_begin, term_land, term_drain = swap(lambda d: term_out.at[d], term_in, term_send, term_recv, slots)

    for load in loads[:2]:
        load.wait()
    owner = owner_ref[...]
    mine = owner == iota((count, blocks), 0)
    before = ones_where(iota((blocks, blocks), 0) < iota((blocks, blocks), 1)).astype(jnp.bfloat16)
    rank = dot(ones_where(mine).astype(jnp.bfloat16), before)
    target = jnp.where(mine, iota((count, blocks), 0).astype(jnp.float32) * PAD + rank, 0.0)
    slot = jnp.sum(target, axis=0, keepdims=True)
    tile = tile_ref[...]
    column = (tile // per_column + 1).astype(jnp.float32)
    inside = lax.rem(tile, per_column).astype(jnp.float32)
    lane = iota((count, LANES), 1)
    packed = jnp.zeros((count, LANES), jnp.float32)
    for s in range(slots):
        here = mine & (rank == float(s))
        for at, what in ((s, column), (PAD + s, inside)):
            found = jnp.sum(jnp.where(here, what, 0.0), axis=1, keepdims=True)
            packed = jnp.where(lane == at, found, packed)
    lists = packed[:lats]
    for s in range(1, sections):
        lists = lists + pltpu.roll(packed[s * lats : (s + 1) * lats], s * 2 * PAD, 1)
    for b in range(lats):
        ids_out[b] = lists[b : b + 1]
    state_in[...] = jnp.zeros_like(state_in)
    term_in[...] = jnp.zeros_like(term_in)
    pl.semaphore_wait(barrier, count - 1)
    ids_begin()

    def kappa_copy(j):
        to = lax.rem(section + j, sections)
        return remote(coded.at[to], kappa.at[section], kappa_send.at[j], kappa_recv.at[j], (to, band))

    def kappa_arrival(j):
        source = lax.rem(section + sections - j, sections)
        return remote(coded.at[source], kappa.at[source], kappa_send.at[j], kappa_recv.at[j], (source, band))

    def row_down(j):
        to = lax.rem(section + j, sections)
        return remote(coded.at[to, :, 0], kappa_high.at[section], down_send.at[j], down_recv.at[j], (to, band - 1))

    def row_up(j):
        to = lax.rem(section + j, sections)
        return remote(coded.at[to, :, rows - 1], kappa_low.at[section], up_send.at[j], up_recv.at[j], (to, band + 1))

    def from_high(j):
        source = lax.rem(section + sections - j, sections)
        return remote(coded.at[source, :, 0], kappa_high.at[source], down_send.at[j], down_recv.at[j], (source, band))

    def from_low(j):
        source = lax.rem(section + sections - j, sections)
        return remote(coded.at[source, :, 0], kappa_low.at[source], up_send.at[j], up_recv.at[j], (source, band))

    def share_kappa():
        for j in range(1, sections):
            kappa_copy(j).start()

    def share_rows(first, stop):
        @pl.when(has_low)
        def _():
            for j in range(first, stop):
                row_down(j).start()

        @pl.when(has_high)
        def _():
            for j in range(first, stop):
                row_up(j).start()

    loads[2].wait()

    def encode(q, carry):
        for c in range(chunks):
            at = pl.multiple_of(q * part + c * CHUNK, CHUNK)
            for r in range(rows):
                scaled = coeff[r, pl.ds(at, CHUNK), :] * SCALE + 0.5
                coded[q, c, r] = scaled.astype(jnp.int32).astype(jnp.int16)
        return carry

    lax.fori_loop(0, sections, encode, 0)
    is_odd = lax.rem(section, 2) == lax.rem(last, 2)

    @pl.when(is_odd)
    def _():
        share_kappa()
        share_rows(0, sections)

    @pl.when(jnp.logical_not(is_odd))
    def _():
        share_rows(0, 1)

    kappa[section] = coded[section]

    holds = ones_where(iota((total, blocks), 0).astype(jnp.float32) == slot)
    place[...] = holds.astype(jnp.bfloat16)
    place_t[...] = holds.T.astype(jnp.bfloat16)

    @pl.when(jnp.logical_not(has_low))
    def _():
        low[...] = jnp.zeros_like(low)
        kappa_low[...] = jnp.zeros_like(kappa_low)

    @pl.when(jnp.logical_not(has_high))
    def _():
        high[...] = jnp.zeros_like(high)
        kappa_high[...] = jnp.zeros_like(kappa_high)

    order = iota((tile_len, tile_len), 0)
    other = iota((tile_len, tile_len), 1)

    def by_part(a, b, size):
        level = a // TW
        place_of = (level // size) * (size * TW) + lax.rem(a, TW) * size + lax.rem(level, size)
        return ones_where(place_of == b).astype(jnp.bfloat16)

    to_parts, from_parts = by_part(order, other, part), by_part(other, order, levels)

    loads[3].wait()
    even = lax.rem(iota((levels, nlon), 1), TW)

    def field(r, carry):
        values = traj[r]
        top = values.astype(jnp.bfloat16).astype(jnp.float32)
        parts = [jnp.where(even == p, x, 0.0) for x in (top, values - top) for p in range(TW)]
        stack = jnp.concatenate(parts, axis=0).T.astype(jnp.bfloat16)
        fields[r] = jnp.concatenate(
            [dot(stack[:, :tile_len], from_parts), dot(stack[:, tile_len:], from_parts)], axis=1
        ).astype(jnp.bfloat16)
        return carry

    lax.fori_loop(0, rows, field, 0)

    ids_land()
    ids = jnp.concatenate([ids_in[d] for d in range(count)], axis=0).astype(jnp.bfloat16)
    source = ones_where(iota((total, count), 0) // PAD == iota((total, count), 1)).astype(jnp.bfloat16)
    spread = dot(source, ids)
    nth = lax.rem(iota((total, LANES), 0), PAD)
    lanes = iota((total, LANES), 1)

    def listed(s):
        at = nth + s * 2 * PAD
        outer = jnp.sum(jnp.where(lanes == at, spread, 0.0), axis=1, keepdims=True)
        inner = jnp.sum(jnp.where(lanes == at + PAD, spread, 0.0), axis=1, keepdims=True)
        which[s] = jnp.broadcast_to(outer, (total, LANES)).astype(jnp.bfloat16)
        pair[s] = ones_where((lanes // TW).astype(jnp.float32) == inner).astype(jnp.bfloat16)

    nothing = jnp.zeros((total, LANES), jnp.bfloat16)

    def tiles(s, r, c):
        return jnp.where(which[s] == jnp.bfloat16(r * columns + c + 1), pair[s], nothing)

    listed(section)
    gathered = jnp.zeros((total, 2 * tile_len), jnp.float32)
    for r in range(rows):
        for c in range(columns):
            chosen[r, :, c * LANES : (c + 1) * LANES] = tiles(section, r, c)
        gathered = gathered + dot(chosen[r], fields[r])
    states = gathered[:, :tile_len] + gathered[:, tile_len:]
    state_out[...] = states.reshape(count, PAD, tile_len)
    state_begin()

    @pl.when(jnp.logical_not(is_odd))
    def _():
        share_kappa()
        share_rows(1, sections)

    for load in loads[4:]:
        load.wait()

    def turn(k, carry):
        jac_t[k] = jac[k].astype(jnp.float32).T.astype(jnp.bfloat16)
        return carry

    lax.fori_loop(0, blocks, turn, 0, unroll=4)

    def list_other(j, carry):
        listed(lax.rem(section + j, sections))
        return carry

    lax.fori_loop(1, sections, list_other, 0)

    def downward(s, c):
        return remote(edge_low.at[s, c], high.at[s, c], low_send.at[s, c], high_recv.at[s, c], (section, band - 1))

    def upward(s, c):
        return remote(edge_high.at[s, c], low.at[s, c], high_send.at[s, c], low_recv.at[s, c], (section, band + 1))

    def along(mid):
        return pltpu.roll(mid, 1, 1) + pltpu.roll(mid, nlon - 1, 1) - 4.0 * mid

    def decode(x):
        return x.astype(jnp.int32).astype(jnp.float32) * (1.0 / SCALE)

    def begin(s, c):
        end = rows - 1

        def weigh(r):
            weighted[c, r] = decode(kappa[s, c, r]) * main[s + 1, c, r].astype(jnp.float32)

        def inner(r):
            value = main[s + 1, c, r].astype(jnp.float32) + along(weighted[c, r])
            if r > 0:
                value = value + weighted[c, r - 1]
            if r < end:
                value = value + weighted[c, r + 1]
            partial[c, r] = value

        for r, near, ref, there, copy in (
            (0, 1, edge_low, has_low, downward), (end, end - 1, edge_high, has_high, upward)
        ):
            weigh(r)
            weigh(near)
            inner(r)
            ref[s, c, 0] = weighted[c, r].astype(jnp.bfloat16)
            ref[s, c, 1] = (decode(kappa[s, c, r]) * partial[c, r]).astype(jnp.bfloat16)

            @pl.when(there)
            def _(copy=copy):
                copy(s, c).start()

        for r in range(2, end - 1):
            weigh(r)
        for r in range(1, end):
            inner(r)

    def complete(s, c, store):
        @pl.when(has_low)
        def _():
            upward(s, c).wait_recv()

        @pl.when(has_high)
        def _():
            downward(s, c).wait_recv()

        end = rows - 1
        partial[c, 0] = partial[c, 0] + low[s, c, 0].astype(jnp.float32)
        partial[c, end] = partial[c, end] + high[s, c, 0].astype(jnp.float32)
        second[0] = low[s, c, 1].astype(jnp.float32) + decode(kappa_low[s, c]) * weighted[c, 0]
        second[rows + 1] = high[s, c, 1].astype(jnp.float32) + decode(kappa_high[s, c]) * weighted[c, end]
        for r in range(rows):
            second[r + 1] = decode(kappa[s, c, r]) * partial[c, r]
        for r in range(rows):
            store(r, partial[c, r] + second[r] + second[r + 2] + along(second[r + 1]))

    def spot(q, c, r):
        return out_ref.at[r, pl.ds(pl.multiple_of(q * part + c * CHUNK, CHUNK), CHUNK), :]

    def give(s, c, r):
        where = (s, band)
        return remote(main.at[s, c, r], spot(section, c, r), out_send.at[s, c, r], out_recv.at[section, c, r], where)

    def taken(q, c, r):
        return remote(main.at[q, c, r], spot(q, c, r), out_send.at[q, c, r], out_recv.at[q, c, r], (q, band))

    def keep_own(c, r):
        return pltpu.make_async_copy(main.at[section, c, r], spot(section, c, r), own_sem.at[c, r])

    def finish(s, c, r, value):
        main[s, c, r] = value.astype(jnp.bfloat16)

    def deliver(s, c):
        @pl.when(s != section)
        def _():
            for r in range(rows):
                give(s, c, r).start()

        @pl.when(s == section)
        def _():
            for r in range(rows):
                keep_own(c, r).start()

    last_from = lax.rem(section + 1, sections)

    @pl.when(last_from != 0)
    def _():
        kappa_arrival(last_from).wait_recv()

    for c in range(chunks):
        end_load(c).wait()

    def open_last(c, carry):
        begin(last, c)
        return carry

    lax.fori_loop(0, chunks, open_last, 0)

    state_land()
    top, rest = split(state_in[...].reshape(total, tile_len))
    top, rest = dot(place_t[...], top), dot(place_t[...], rest)
    groups = blocks // PAD
    for g in range(groups):
        span = slice(g * PAD, (g + 1) * PAD)
        state_rows[g] = jnp.concatenate([top[span], rest[span]], axis=0).astype(jnp.bfloat16)
    among = lax.rem(iota((2 * PAD, tile_len), 0), PAD)

    def product(both, mats, g):
        picked = jnp.zeros((2 * PAD, tile_len), jnp.float32)
        for i in range(PAD):
            picked = jnp.where(among == i, dot(both, mats[g * PAD + i]), picked)
        return picked[:PAD] + picked[PAD:]

    for g in range(groups):
        here = slice(g * PAD, (g + 1) * PAD)
        pred = product(state_rows[g], jac_t, g)
        weight = weight_ref[here, :] * valid_ref[here, :].astype(jnp.float32)
        resid = weight * (value_ref[here, :] - pred)
        top = resid.astype(jnp.bfloat16).astype(jnp.float32)
        resid_rows[g] = jnp.concatenate([top, resid - top], axis=0).astype(jnp.bfloat16)
    for g in range(groups):
        terms[g * PAD : (g + 1) * PAD, :] = product(resid_rows[g], jac, g)
    top, rest = split(terms[...])
    top, rest = dot(top, to_parts).astype(jnp.bfloat16), dot(rest, to_parts).astype(jnp.bfloat16)
    sent = dot(place[...], top) + dot(place[...], rest)
    group = lats * PAD
    strip = iota((group, tile_len), 1) // width
    for q in range(sections):
        parcel = jnp.zeros((group, tile_len), jnp.float32)
        for s in range(sections):
            moved = sent[s * group : (s + 1) * group]
            if s != q:
                moved = pltpu.roll(moved, ((s - q) % sections) * width, 1)
            parcel = jnp.where(strip == s, moved, parcel)
        term_out[q * lats : (q + 1) * lats] = parcel.reshape(lats, PAD, tile_len)
    term_begin()
    ids_drain()
    state_drain()

    for j in range(sections):
        @pl.when(has_high)
        def _(j=j):
            from_high(j).wait_recv()

        @pl.when(has_low)
        def _(j=j):
            from_low(j).wait_recv()

    def kappa_land(j, carry):
        @pl.when(j != last_from)
        def _():
            kappa_arrival(j).wait_recv()

        return carry

    lax.fori_loop(1, sections, kappa_land, 0)

    def close_last(c, carry):
        def keep(r, value):
            early[c, r] = value

        complete(last, c, keep)
        return carry

    lax.fori_loop(0, chunks, close_last, 0)

    term_land()
    got = term_in[...].reshape(total, tile_len).T
    top = got.astype(jnp.bfloat16).astype(jnp.float32)
    rest = got - top
    for s in range(sections):
        span = slice(s * width, (s + 1) * width)
        stack = jnp.concatenate([top[span], rest[span]], axis=0).astype(jnp.bfloat16)
        terms_t[s] = stack
    wide = 2 * LANES
    parity = lax.rem(iota((part, wide), 1), TW)

    def scatter(s):
        left = terms_t[s]
        for r in range(rows):
            for c in range(nlon // wide):
                right = jnp.concatenate([tiles(s, r, 2 * c), tiles(s, r, 2 * c + 1)], axis=1)
                both = dot(left, right)
                both = both[:width] + both[width:]
                value = jnp.where(parity == 0, both[:part], both[part:])
                for k in range(chunks):
                    forcing[s, k, r, :, c * wide : (c + 1) * wide] = value[k * CHUNK : (k + 1) * CHUNK]

    scatter(last)

    def start_last(c, carry):
        for r in range(rows):
            finish(last, c, r, early[c, r] + forcing[last, c, r])
        if last > 0:
            begin(last - 1, c)
        deliver(last, c)
        return carry

    lax.fori_loop(0, chunks, start_last, 0)

    def scatter_other(j, carry):
        scatter(last - j)
        return carry

    lax.fori_loop(1, sections, scatter_other, 0)

    def go(i, carry):
        s = last - 1 - i // chunks
        c = lax.rem(i, chunks)
        complete(s, c, lambda r, value: finish(s, c, r, value + forcing[s, c, r]))

        @pl.when(s > 0)
        def _():
            begin(s - 1, c)

        deliver(s, c)
        return carry

    lax.fori_loop(0, last * chunks, go, 0)

    term_drain()
    for j in range(1, sections):
        kappa_copy(j).wait_send()
    for cond, copy in ((has_low, row_down), (has_high, row_up)):
        @pl.when(cond)
        def _(copy=copy):
            for j in range(sections):
                copy(j).wait_send()

    def settle(i, carry):
        s, c = i // chunks, lax.rem(i, chunks)

        @pl.when(has_low)
        def _():
            downward(s, c).wait_send()

        @pl.when(has_high)
        def _():
            upward(s, c).wait_send()

        @pl.when(s != section)
        def _():
            for r in range(rows):
                give(s, c, r).wait_send()

        @pl.when(s == section)
        def _():
            for r in range(rows):
                keep_own(c, r).wait()

        return carry

    lax.fori_loop(0, sections * chunks, settle, 0)

    def gain(i, carry):
        q, c = lax.rem(section + 1 + i // chunks, sections), lax.rem(i, chunks)
        for r in range(rows):
            taken(q, c, r).wait_recv()
        return carry

    lax.fori_loop(0, last * chunks, gain, 0)


def sweep(owner, tile, value, weight, valid, traj, coeff, end, jac, slots):
    lats, sections = lax.axis_size("lat"), lax.axis_size("tm")
    count = sections * lats
    _, rows, levels, nlon = traj.shape
    blocks = owner.shape[1]
    tile_len = levels * TW
    total = count * PAD
    chunks = levels // sections // CHUNK
    bf16, f32 = jnp.bfloat16, jnp.float32
    parcels = pltpu.VMEM((count, PAD, tile_len), f32)
    stacked = pltpu.VMEM((blocks // PAD, 2 * PAD, tile_len), bf16)
    work = pltpu.VMEM((chunks, rows, CHUNK, nlon), f32)
    edges = pltpu.VMEM((sections, chunks, SUB, CHUNK, nlon), bf16)
    codes = lambda *lead: pltpu.VMEM(lead + (CHUNK, nlon), jnp.int16)
    hbm = pl.BlockSpec(memory_space=pltpu.HBM)
    dma = pltpu.SemaphoreType.DMA
    return pl.pallas_call(
        functools.partial(sweep_kernel, lats, sections, slots),
        out_shape=jax.ShapeDtypeStruct((rows, levels, nlon), bf16),
        in_specs=[hbm] * 9,
        out_specs=hbm,
        scratch_shapes=[
            pltpu.VMEM(owner.shape, owner.dtype),
            pltpu.VMEM(tile.shape, tile.dtype),
            pltpu.VMEM(value.shape, value.dtype),
            pltpu.VMEM(weight.shape, weight.dtype),
            pltpu.VMEM(valid.shape, valid.dtype),
            pltpu.VMEM((rows, levels, nlon), f32),
            pltpu.VMEM((rows, levels, nlon), f32),
            pltpu.VMEM(jac.shape, bf16),
            pltpu.VMEM(jac.shape, bf16),
            pltpu.VMEM((rows, nlon, 2 * tile_len), bf16),
            pltpu.VMEM((rows, total, nlon), bf16),
            pltpu.VMEM((total, blocks), bf16),
            pltpu.VMEM((blocks, total), bf16),
            pltpu.VMEM((sections, total, LANES), bf16),
            pltpu.VMEM((sections, total, LANES), bf16),
            pltpu.VMEM((lats, 1, LANES), f32),
            pltpu.VMEM((count, 1, LANES), f32),
            parcels, parcels, parcels, parcels, stacked, stacked,
            pltpu.VMEM((blocks, tile_len), f32),
            pltpu.VMEM((sections, 2 * tile_len // sections, total), bf16),
            codes(sections, chunks, rows),
            codes(sections, chunks, rows),
            codes(sections, chunks),
            codes(sections, chunks),
            pltpu.VMEM((sections + 1, chunks, rows, CHUNK, nlon), bf16),
            pltpu.VMEM((sections, chunks, rows, CHUNK, nlon), f32),
            work, work,
            pltpu.VMEM((rows + 2, CHUNK, nlon), f32),
            work,
            edges, edges, edges, edges,
            dma((8,)),
            dma((chunks,)),
        ]
        + [dma((count,))] * 6
        + [dma((sections,))] * 6
        + [dma((sections, chunks))] * 4
        + [dma((sections, chunks, rows))] * 2
        + [dma((chunks, rows))],
        compiler_params=pltpu.CompilerParams(
            collective_id=1, has_side_effects=True, vmem_limit_bytes=63 * 1024 * 1024
        ),
        name="sweep",
    )(owner, tile, value, weight, valid, traj, coeff, end, jac)


def widen_kernel(x_hbm, out_hbm, x, wide, in_sem, out_sem):
    rows = x.shape[0]

    def load(r):
        return pltpu.make_async_copy(x_hbm.at[r], x.at[r], in_sem.at[r])

    def save(r):
        return pltpu.make_async_copy(wide.at[r], out_hbm.at[0, r], out_sem.at[r])

    for r in range(rows):
        load(r).start()
    for r in range(rows):
        load(r).wait()
        wide[r] = x[r].astype(jnp.float32)
        save(r).start()
    for r in range(rows):
        save(r).wait()


def widen(x):
    hbm = pl.BlockSpec(memory_space=pltpu.HBM)
    dma = pltpu.SemaphoreType.DMA((x.shape[0],))
    return pl.pallas_call(
        widen_kernel,
        out_shape=jax.ShapeDtypeStruct((1,) + x.shape, jnp.float32),
        in_specs=[hbm],
        out_specs=hbm,
        scratch_shapes=[pltpu.VMEM(x.shape, x.dtype), pltpu.VMEM(x.shape, jnp.float32), dma, dma],
        compiler_params=pltpu.CompilerParams(vmem_limit_bytes=63 * 1024 * 1024),
        name="widen",
    )(x)


def per_device(
    trajectory,
    diffusivity,
    adjoint_end,
    obs_jac,
    obs_value,
    obs_weight,
    obs_valid,
    obs_owner,
    obs_tile,
):
    devices = lax.axis_size("tm") * lax.axis_size("lat")
    blocks = obs_owner.shape[0]
    slots = max(2, 2 * blocks // devices)
    rounded = sweep(
        obs_owner[:, 0][None, :], obs_tile[None, :], obs_value, obs_weight, obs_valid,
        trajectory, diffusivity, adjoint_end, obs_jac, slots,
    )
    return widen(rounded)


def solution(mesh):
    in_specs = (
        P("tm", "lat", None, None),
        P("tm", "lat", None, None),
        P("lat", None, None),
        P(("tm", "lat"), None, None),
        P(("tm", "lat"), None),
        P(("tm", "lat"), None),
        P(("tm", "lat"), None),
        P(("tm", "lat"), None),
        P(("tm", "lat")),
    )
    out_specs = P("tm", "lat", None, None)
    return jax.shard_map(
        per_device, mesh=mesh, in_specs=in_specs, out_specs=out_specs, check_vma=False
    )
```

```python
import functools

import jax
import jax.numpy as jnp
from jax import lax
from jax.experimental import pallas as pl
from jax.experimental.pallas import tpu as pltpu
from jax.sharding import PartitionSpec as P

TW = 2
SUB = 2
LANES = 128
PAD = 8
CHUNK = 8
SCALE = 2.0**17
MESH = pl.DeviceIdType.MESH
VMEM = pl.BlockSpec(memory_space=pltpu.VMEM)


def split(x):
    top = x.astype(jnp.bfloat16)
    return top, (x - top.astype(jnp.float32)).astype(jnp.bfloat16)


def dot(a, b):
    return jnp.dot(a, b, preferred_element_type=jnp.float32)


def iota(shape, axis):
    return lax.broadcasted_iota(jnp.int32, shape, axis)


def ones_where(mask):
    return jnp.where(mask, 1.0, 0.0)


def sweep_kernel(
    lats, sections, slots,
    owner_hbm, tile_hbm, value_hbm, weight_hbm, valid_hbm, traj_hbm, coeff_hbm, end_hbm, jac_hbm,
    out_ref,
    owner_ref, tile_ref, value_ref, weight_ref, valid_ref, traj, coeff, jac, jac_t, fields, chosen, place, place_t, which, pair,
    ids_out, ids_in, state_out, state_in, term_out, term_in, state_rows, resid_rows, terms, terms_t,
    coded, kappa, kappa_low, kappa_high, main, forcing, weighted, partial, second, early,
    edge_low, edge_high, low, high,
    load_sem, end_sem, ids_send, ids_recv, state_send, state_recv, term_send, term_recv,
    kappa_send, kappa_recv, down_send, down_recv, up_send, up_recv,
    low_send, low_recv, high_send, high_recv, out_send, out_recv, own_sem,
):
    section, band = lax.axis_index("tm"), lax.axis_index("lat")
    count = sections * lats
    me = section * lats + band
    rows, levels, nlon = coeff.shape
    blocks = owner_ref.shape[1]
    total = count * PAD
    columns = nlon // LANES
    per_column = LANES // TW
    tile_len = levels * TW
    part = levels // sections
    chunks = part // CHUNK
    width = part * TW
    has_low, has_high = band > 0, band < lats - 1
    last = sections - 1

    loads = [
        pltpu.make_async_copy(src, dst, load_sem.at[i])
        for i, (src, dst) in enumerate(
            (
                (owner_hbm, owner_ref), (tile_hbm, tile_ref), (coeff_hbm.at[0], coeff), (traj_hbm.at[0], traj),
                (jac_hbm, jac), (value_hbm, value_ref), (weight_hbm, weight_ref), (valid_hbm, valid_ref),
            )
        )
    ]
    for load in loads:
        load.start()

    def end_load(c):
        at = pl.multiple_of(section * part + c * CHUNK, CHUNK)
        return pltpu.make_async_copy(end_hbm.at[:, pl.ds(at, CHUNK), :], main.at[sections, c], end_sem.at[c])

    for c in range(chunks):
        end_load(c).start()

    barrier = pltpu.get_barrier_semaphore()

    def peer(j):
        to = lax.rem(me + j, count)
        return to, (to // lats, lax.rem(to, lats))

    def nearer(i):
        far = lats - 1 - i // 2
        lat = jnp.where(lax.rem(i, 2) == 0, band + far, band - far)
        return far, lat, (lat >= 0) & (lat < lats) & ((far > 0) | (lax.rem(i, 2) == 0))

    def greet(i, carry):
        far, lat, inside = nearer(i)

        @pl.when(inside)
        def _():
            def one(j, carry):
                where = (lax.rem(section + sections - j, sections), lat)
                pl.semaphore_signal(barrier, inc=1, device_id=where, device_id_type=MESH)
                return carry

            lax.fori_loop(1, jnp.where(far > 0, sections + 1, sections), one, 0)

        return carry

    lax.fori_loop(0, 2 * lats, greet, 0)

    def remote(src, dst, send, recv, where):
        return pltpu.make_async_remote_copy(
            src_ref=src, dst_ref=dst, send_sem=send, recv_sem=recv, device_id=where, device_id_type=MESH
        )

    def swap(pick, into, send, recv, used):
        def outgoing(to):
            where = (to // lats, lax.rem(to, lats))
            return remote(pick(to).at[:used], into.at[me, :used], send.at[to], recv.at[me], where)

        def incoming(source):
            where = (source // lats, lax.rem(source, lats))
            return remote(pick(source).at[:used], into.at[source, :used], send.at[source], recv.at[source], where)

        def launch(i, carry):
            far, lat, inside = nearer(i)

            @pl.when(inside)
            def _():
                def one(j, carry):
                    outgoing(lax.rem(section + sections - j, sections) * lats + lat).start()
                    return carry

                lax.fori_loop(1, jnp.where(far > 0, sections + 1, sections), one, 0)

            return carry

        def land(j, carry):
            incoming(lax.rem(me + count - j, count)).wait_recv()
            return carry

        def drain(j, carry):
            outgoing(lax.rem(me + j, count)).wait_send()
            return carry

        def begin():
            lax.fori_loop(0, 2 * lats, launch, 0)
            into[me] = pick(me)[...]

        return begin, lambda: lax.fori_loop(1, count, land, 0), lambda: lax.fori_loop(1, count, drain, 0)

    ids_begin, ids_land, ids_drain = swap(lambda d: ids_out.at[lax.rem(d, lats)], ids_in, ids_send, ids_recv, 1)
    state_begin, state_land, state_drain = swap(lambda d: state_out.at[d], state_in, state_send, state_recv, slots)
    term_begin, term_land, term_drain = swap(lambda d: term_out.at[d], term_in, term_send, term_recv, slots)

    for load in loads[:2]:
        load.wait()
    owner = owner_ref[...]
    mine = owner == iota((count, blocks), 0)
    before = ones_where(iota((blocks, blocks), 0) < iota((blocks, blocks), 1)).astype(jnp.bfloat16)
    rank = dot(ones_where(mine).astype(jnp.bfloat16), before)
    target = jnp.where(mine, iota((count, blocks), 0).astype(jnp.float32) * PAD + rank, 0.0)
    slot = jnp.sum(target, axis=0, keepdims=True)
    tile = tile_ref[...]
    column = (tile // per_column + 1).astype(jnp.float32)
    inside = lax.rem(tile, per_column).astype(jnp.float32)
    lane = iota((count, LANES), 1)
    packed = jnp.zeros((count, LANES), jnp.float32)
    for s in range(slots):
        here = mine & (rank == float(s))
        for at, what in ((s, column), (PAD + s, inside)):
            found = jnp.sum(jnp.where(here, what, 0.0), axis=1, keepdims=True)
            packed = jnp.where(lane == at, found, packed)
    lists = packed[:lats]
    for s in range(1, sections):
        lists = lists + pltpu.roll(packed[s * lats : (s + 1) * lats], s * 2 * PAD, 1)
    for b in range(lats):
        ids_out[b] = lists[b : b + 1]
    state_in[...] = jnp.zeros_like(state_in)
    term_in[...] = jnp.zeros_like(term_in)
    pl.semaphore_wait(barrier, count - 1)
    ids_begin()

    def kappa_copy(j):
        to = lax.rem(section + j, sections)
        return remote(coded.at[to], kappa.at[section], kappa_send.at[j], kappa_recv.at[j], (to, band))

    def kappa_arrival(j):
        source = lax.rem(section + sections - j, sections)
        return remote(coded.at[source], kappa.at[source], kappa_send.at[j], kappa_recv.at[j], (source, band))

    def row_down(j):
        to = lax.rem(section + j, sections)
        return remote(coded.at[to, :, 0], kappa_high.at[section], down_send.at[j], down_recv.at[j], (to, band - 1))

    def row_up(j):
        to = lax.rem(section + j, sections)
        return remote(coded.at[to, :, rows - 1], kappa_low.at[section], up_send.at[j], up_recv.at[j], (to, band + 1))

    def from_high(j):
        source = lax.rem(section + sections - j, sections)
        return remote(coded.at[source, :, 0], kappa_high.at[source], down_send.at[j], down_recv.at[j], (source, band))

    def from_low(j):
        source = lax.rem(section + sections - j, sections)
        return remote(coded.at[source, :, 0], kappa_low.at[source], up_send.at[j], up_recv.at[j], (source, band))

    def share_kappa():
        for j in range(1, sections):
            kappa_copy(j).start()

    def share_rows(first, stop):
        @pl.when(has_low)
        def _():
            for j in range(first, stop):
                row_down(j).start()

        @pl.when(has_high)
        def _():
            for j in range(first, stop):
                row_up(j).start()

    loads[2].wait()

    def encode(q, carry):
        for c in range(chunks):
            at = pl.multiple_of(q * part + c * CHUNK, CHUNK)
            for r in range(rows):
                scaled = coeff[r, pl.ds(at, CHUNK), :] * SCALE + 0.5
                coded[q, c, r] = scaled.astype(jnp.int32).astype(jnp.int16)
        return carry

    lax.fori_loop(0, sections, encode, 0)
    is_odd = lax.rem(section, 2) == lax.rem(last, 2)

    @pl.when(is_odd)
    def _():
        share_kappa()
        share_rows(0, sections)

    @pl.when(jnp.logical_not(is_odd))
    def _():
        share_rows(0, 1)

    kappa[section] = coded[section]

    holds = ones_where(iota((total, blocks), 0).astype(jnp.float32) == slot)
    place[...] = holds.astype(jnp.bfloat16)
    place_t[...] = holds.T.astype(jnp.bfloat16)

    @pl.when(jnp.logical_not(has_low))
    def _():
        low[...] = jnp.zeros_like(low)
        kappa_low[...] = jnp.zeros_like(kappa_low)

    @pl.when(jnp.logical_not(has_high))
    def _():
        high[...] = jnp.zeros_like(high)
        kappa_high[...] = jnp.zeros_like(kappa_high)

    order = iota((tile_len, tile_len), 0)
    other = iota((tile_len, tile_len), 1)

    def by_part(a, b, size):
        level = a // TW
        place_of = (level // size) * (size * TW) + lax.rem(a, TW) * size + lax.rem(level, size)
        return ones_where(place_of == b).astype(jnp.bfloat16)

    to_parts, from_parts = by_part(order, other, part), by_part(other, order, levels)

    loads[3].wait()
    even = lax.rem(iota((levels, nlon), 1), TW)

    def field(r, carry):
        values = traj[r]
        top = values.astype(jnp.bfloat16).astype(jnp.float32)
        parts = [jnp.where(even == p, x, 0.0) for x in (top, values - top) for p in range(TW)]
        stack = jnp.concatenate(parts, axis=0).T.astype(jnp.bfloat16)
        fields[r] = jnp.concatenate(
            [dot(stack[:, :tile_len], from_parts), dot(stack[:, tile_len:], from_parts)], axis=1
        ).astype(jnp.bfloat16)
        return carry

    lax.fori_loop(0, rows, field, 0)

    ids_land()
    ids = jnp.concatenate([ids_in[d] for d in range(count)], axis=0).astype(jnp.bfloat16)
    source = ones_where(iota((total, count), 0) // PAD == iota((total, count), 1)).astype(jnp.bfloat16)
    spread = dot(source, ids)
    nth = lax.rem(iota((total, LANES), 0), PAD)
    lanes = iota((total, LANES), 1)

    def listed(s):
        at = nth + s * 2 * PAD
        outer = jnp.sum(jnp.where(lanes == at, spread, 0.0), axis=1, keepdims=True)
        inner = jnp.sum(jnp.where(lanes == at + PAD, spread, 0.0), axis=1, keepdims=True)
        which[s] = jnp.broadcast_to(outer, (total, LANES)).astype(jnp.bfloat16)
        pair[s] = ones_where((lanes // TW).astype(jnp.float32) == inner).astype(jnp.bfloat16)

    nothing = jnp.zeros((total, LANES), jnp.bfloat16)

    def tiles(s, r, c):
        return jnp.where(which[s] == jnp.bfloat16(r * columns + c + 1), pair[s], nothing)

    listed(section)
    gathered = jnp.zeros((total, 2 * tile_len), jnp.float32)
    for r in range(rows):
        for c in range(columns):
            chosen[r, :, c * LANES : (c + 1) * LANES] = tiles(section, r, c)
        gathered = gathered + dot(chosen[r], fields[r])
    states = gathered[:, :tile_len] + gathered[:, tile_len:]
    state_out[...] = states.reshape(count, PAD, tile_len)
    state_begin()

    @pl.when(jnp.logical_not(is_odd))
    def _():
        share_kappa()
        share_rows(1, sections)

    for load in loads[4:]:
        load.wait()

    def turn(k, carry):
        jac_t[k] = jac[k].astype(jnp.float32).T.astype(jnp.bfloat16)
        return carry

    lax.fori_loop(0, blocks, turn, 0, unroll=4)

    def downward(s, c):
        return remote(edge_low.at[s, c], high.at[s, c], low_send.at[s, c], high_recv.at[s, c], (section, band - 1))

    def upward(s, c):
        return remote(edge_high.at[s, c], low.at[s, c], high_send.at[s, c], low_recv.at[s, c], (section, band + 1))

    def along(mid):
        return pltpu.roll(mid, 1, 1) + pltpu.roll(mid, nlon - 1, 1) - 4.0 * mid

    def decode(x):
        return x.astype(jnp.int32).astype(jnp.float32) * (1.0 / SCALE)

    def begin(s, c):
        end = rows - 1

        def weigh(r):
            weighted[c, r] = decode(kappa[s, c, r]) * main[s + 1, c, r].astype(jnp.float32)

        def inner(r):
            value = main[s + 1, c, r].astype(jnp.float32) + along(weighted[c, r])
            if r > 0:
                value = value + weighted[c, r - 1]
            if r < end:
                value = value + weighted[c, r + 1]
            partial[c, r] = value

        for r, near, ref, there, copy in (
            (0, 1, edge_low, has_low, downward), (end, end - 1, edge_high, has_high, upward)
        ):
            weigh(r)
            weigh(near)
            inner(r)
            ref[s, c, 0] = weighted[c, r].astype(jnp.bfloat16)
            ref[s, c, 1] = (decode(kappa[s, c, r]) * partial[c, r]).astype(jnp.bfloat16)

            @pl.when(there)
            def _(copy=copy):
                copy(s, c).start()

        for r in range(2, end - 1):
            weigh(r)
        for r in range(1, end):
            inner(r)

    def complete(s, c, store):
        @pl.when(has_low)
        def _():
            upward(s, c).wait_recv()

        @pl.when(has_high)
        def _():
            downward(s, c).wait_recv()

        end = rows - 1
        partial[c, 0] = partial[c, 0] + low[s, c, 0].astype(jnp.float32)
        partial[c, end] = partial[c, end] + high[s, c, 0].astype(jnp.float32)
        second[0] = low[s, c, 1].astype(jnp.float32) + decode(kappa_low[s, c]) * weighted[c, 0]
        second[rows + 1] = high[s, c, 1].astype(jnp.float32) + decode(kappa_high[s, c]) * weighted[c, end]
        for r in range(rows):
            second[r + 1] = decode(kappa[s, c, r]) * partial[c, r]
        for r in range(rows):
            store(r, partial[c, r] + second[r] + second[r + 2] + along(second[r + 1]))

    def spot(q, c, r):
        return out_ref.at[r, pl.ds(pl.multiple_of(q * part + c * CHUNK, CHUNK), CHUNK), :]

    def give(s, c, r):
        where = (s, band)
        return remote(main.at[s, c, r], spot(section, c, r), out_send.at[s, c, r], out_recv.at[section, c, r], where)

    def taken(q, c, r):
        return remote(main.at[q, c, r], spot(q, c, r), out_send.at[q, c, r], out_recv.at[q, c, r], (q, band))

    def keep_own(c, r):
        return pltpu.make_async_copy(main.at[section, c, r], spot(section, c, r), own_sem.at[c, r])

    def finish(s, c, r, value):
        main[s, c, r] = value.astype(jnp.bfloat16)

    def deliver(s, c):
        @pl.when(s != section)
        def _():
            for r in range(rows):
                give(s, c, r).start()

        @pl.when(s == section)
        def _():
            for r in range(rows):
                keep_own(c, r).start()

    last_from = lax.rem(section + 1, sections)

    @pl.when(last_from != 0)
    def _():
        kappa_arrival(last_from).wait_recv()

    for c in range(chunks):
        end_load(c).wait()

    def open_last(c, carry):
        begin(last, c)
        return carry

    lax.fori_loop(0, chunks, open_last, 0)

    state_land()
    top, rest = split(state_in[...].reshape(total, tile_len))
    top, rest = dot(place_t[...], top), dot(place_t[...], rest)
    groups = blocks // PAD
    for g in range(groups):
        span = slice(g * PAD, (g + 1) * PAD)
        state_rows[g] = jnp.concatenate([top[span], rest[span]], axis=0).astype(jnp.bfloat16)
    among = lax.rem(iota((2 * PAD, tile_len), 0), PAD)

    def product(both, mats, g):
        picked = jnp.zeros((2 * PAD, tile_len), jnp.float32)
        for i in range(0, PAD, 2):
            k = g * PAD + i
            full = dot(both, jnp.concatenate([mats[k], mats[k + 1]], axis=1))
            picked = jnp.where(among == i, full[:, :tile_len], picked)
            picked = jnp.where(among == i + 1, full[:, tile_len:], picked)
        return picked[:PAD] + picked[PAD:]

    for g in range(groups):
        here = slice(g * PAD, (g + 1) * PAD)
        pred = product(state_rows[g], jac_t, g)
        weight = weight_ref[here, :] * valid_ref[here, :].astype(jnp.float32)
        resid = weight * (value_ref[here, :] - pred)
        top = resid.astype(jnp.bfloat16).astype(jnp.float32)
        resid_rows[g] = jnp.concatenate([top, resid - top], axis=0).astype(jnp.bfloat16)
    for g in range(groups):
        terms[g * PAD : (g + 1) * PAD, :] = product(resid_rows[g], jac, g)
    top, rest = split(terms[...])
    top, rest = dot(top, to_parts).astype(jnp.bfloat16), dot(rest, to_parts).astype(jnp.bfloat16)
    sent = dot(place[...], top) + dot(place[...], rest)
    group = lats * PAD
    strip = iota((group, tile_len), 1) // width
    for q in range(sections):
        parcel = jnp.zeros((group, tile_len), jnp.float32)
        for s in range(sections):
            moved = sent[s * group : (s + 1) * group]
            if s != q:
                moved = pltpu.roll(moved, ((s - q) % sections) * width, 1)
            parcel = jnp.where(strip == s, moved, parcel)
        term_out[q * lats : (q + 1) * lats] = parcel.reshape(lats, PAD, tile_len)
    term_begin()
    def list_other(j, carry):
        listed(lax.rem(section + j, sections))
        return carry

    lax.fori_loop(1, sections, list_other, 0)

    ids_drain()
    state_drain()

    for j in range(sections):
        @pl.when(has_high)
        def _(j=j):
            from_high(j).wait_recv()

        @pl.when(has_low)
        def _(j=j):
            from_low(j).wait_recv()

    def kappa_land(j, carry):
        @pl.when(j != last_from)
        def _():
            kappa_arrival(j).wait_recv()

        return carry

    lax.fori_loop(1, sections, kappa_land, 0)

    def close_last(c, carry):
        def keep(r, value):
            early[c, r] = value

        complete(last, c, keep)
        return carry

    lax.fori_loop(0, chunks, close_last, 0)

    term_land()
    got = term_in[...].reshape(total, tile_len).T
    top = got.astype(jnp.bfloat16).astype(jnp.float32)
    rest = got - top
    for s in range(sections):
        span = slice(s * width, (s + 1) * width)
        stack = jnp.concatenate([top[span], rest[span]], axis=0).astype(jnp.bfloat16)
        terms_t[s] = stack
    wide = 2 * LANES
    parity = lax.rem(iota((part, wide), 1), TW)

    def scatter(s):
        left = terms_t[s]
        for r in range(rows):
            for c in range(nlon // wide):
                right = jnp.concatenate([tiles(s, r, 2 * c), tiles(s, r, 2 * c + 1)], axis=1)
                both = dot(left, right)
                both = both[:width] + both[width:]
                value = jnp.where(parity == 0, both[:part], both[part:])
                for k in range(chunks):
                    forcing[s, k, r, :, c * wide : (c + 1) * wide] = value[k * CHUNK : (k + 1) * CHUNK]

    scatter(last)

    def start_last(c, carry):
        for r in range(rows):
            finish(last, c, r, early[c, r] + forcing[last, c, r])
        if last > 0:
            begin(last - 1, c)
        deliver(last, c)
        return carry

    lax.fori_loop(0, chunks, start_last, 0)

    def scatter_other(j, carry):
        scatter(last - j)
        return carry

    lax.fori_loop(1, sections, scatter_other, 0)

    def go(i, carry):
        s = last - 1 - i // chunks
        c = lax.rem(i, chunks)
        complete(s, c, lambda r, value: finish(s, c, r, value + forcing[s, c, r]))

        @pl.when(s > 0)
        def _():
            begin(s - 1, c)

        deliver(s, c)
        return carry

    lax.fori_loop(0, last * chunks, go, 0)

    term_drain()
    for j in range(1, sections):
        kappa_copy(j).wait_send()
    for cond, copy in ((has_low, row_down), (has_high, row_up)):
        @pl.when(cond)
        def _(copy=copy):
            for j in range(sections):
                copy(j).wait_send()

    def settle(i, carry):
        s, c = i // chunks, lax.rem(i, chunks)

        @pl.when(has_low)
        def _():
            downward(s, c).wait_send()

        @pl.when(has_high)
        def _():
            upward(s, c).wait_send()

        @pl.when(s != section)
        def _():
            for r in range(rows):
                give(s, c, r).wait_send()

        @pl.when(s == section)
        def _():
            for r in range(rows):
                keep_own(c, r).wait()

        return carry

    lax.fori_loop(0, sections * chunks, settle, 0)

    def gain(i, carry):
        q, c = lax.rem(section + 1 + i // chunks, sections), lax.rem(i, chunks)
        for r in range(rows):
            taken(q, c, r).wait_recv()
        return carry

    lax.fori_loop(0, last * chunks, gain, 0)


def sweep(owner, tile, value, weight, valid, traj, coeff, end, jac, slots):
    lats, sections = lax.axis_size("lat"), lax.axis_size("tm")
    count = sections * lats
    _, rows, levels, nlon = traj.shape
    blocks = owner.shape[1]
    tile_len = levels * TW
    total = count * PAD
    chunks = levels // sections // CHUNK
    bf16, f32 = jnp.bfloat16, jnp.float32
    parcels = pltpu.VMEM((count, PAD, tile_len), f32)
    stacked = pltpu.VMEM((blocks // PAD, 2 * PAD, tile_len), bf16)
    work = pltpu.VMEM((chunks, rows, CHUNK, nlon), f32)
    edges = pltpu.VMEM((sections, chunks, SUB, CHUNK, nlon), bf16)
    codes = lambda *lead: pltpu.VMEM(lead + (CHUNK, nlon), jnp.int16)
    hbm = pl.BlockSpec(memory_space=pltpu.HBM)
    dma = pltpu.SemaphoreType.DMA
    return pl.pallas_call(
        functools.partial(sweep_kernel, lats, sections, slots),
        out_shape=jax.ShapeDtypeStruct((rows, levels, nlon), bf16),
        in_specs=[hbm] * 9,
        out_specs=hbm,
        scratch_shapes=[
            pltpu.VMEM(owner.shape, owner.dtype),
            pltpu.VMEM(tile.shape, tile.dtype),
            pltpu.VMEM(value.shape, value.dtype),
            pltpu.VMEM(weight.shape, weight.dtype),
            pltpu.VMEM(valid.shape, valid.dtype),
            pltpu.VMEM((rows, levels, nlon), f32),
            pltpu.VMEM((rows, levels, nlon), f32),
            pltpu.VMEM(jac.shape, bf16),
            pltpu.VMEM(jac.shape, bf16),
            pltpu.VMEM((rows, nlon, 2 * tile_len), bf16),
            pltpu.VMEM((rows, total, nlon), bf16),
            pltpu.VMEM((total, blocks), bf16),
            pltpu.VMEM((blocks, total), bf16),
            pltpu.VMEM((sections, total, LANES), bf16),
            pltpu.VMEM((sections, total, LANES), bf16),
            pltpu.VMEM((lats, 1, LANES), f32),
            pltpu.VMEM((count, 1, LANES), f32),
            parcels, parcels, parcels, parcels, stacked, stacked,
            pltpu.VMEM((blocks, tile_len), f32),
            pltpu.VMEM((sections, 2 * tile_len // sections, total), bf16),
            codes(sections, chunks, rows),
            codes(sections, chunks, rows),
            codes(sections, chunks),
            codes(sections, chunks),
            pltpu.VMEM((sections + 1, chunks, rows, CHUNK, nlon), bf16),
            pltpu.VMEM((sections, chunks, rows, CHUNK, nlon), f32),
            work, work,
            pltpu.VMEM((rows + 2, CHUNK, nlon), f32),
            work,
            edges, edges, edges, edges,
            dma((8,)),
            dma((chunks,)),
        ]
        + [dma((count,))] * 6
        + [dma((sections,))] * 6
        + [dma((sections, chunks))] * 4
        + [dma((sections, chunks, rows))] * 2
        + [dma((chunks, rows))],
        compiler_params=pltpu.CompilerParams(
            collective_id=1, has_side_effects=True, vmem_limit_bytes=63 * 1024 * 1024
        ),
        name="sweep",
    )(owner, tile, value, weight, valid, traj, coeff, end, jac)


def widen_kernel(x_hbm, out_hbm, x, wide, in_sem, out_sem):
    rows = x.shape[0]

    def load(r):
        return pltpu.make_async_copy(x_hbm.at[r], x.at[r], in_sem.at[r])

    def save(r):
        return pltpu.make_async_copy(wide.at[r], out_hbm.at[0, r], out_sem.at[r])

    for r in range(rows):
        load(r).start()
    for r in range(rows):
        load(r).wait()
        wide[r] = x[r].astype(jnp.float32)
        save(r).start()
    for r in range(rows):
        save(r).wait()


def widen(x):
    hbm = pl.BlockSpec(memory_space=pltpu.HBM)
    dma = pltpu.SemaphoreType.DMA((x.shape[0],))
    return pl.pallas_call(
        widen_kernel,
        out_shape=jax.ShapeDtypeStruct((1,) + x.shape, jnp.float32),
        in_specs=[hbm],
        out_specs=hbm,
        scratch_shapes=[pltpu.VMEM(x.shape, x.dtype), pltpu.VMEM(x.shape, jnp.float32), dma, dma],
        compiler_params=pltpu.CompilerParams(vmem_limit_bytes=63 * 1024 * 1024),
        name="widen",
    )(x)


def per_device(
    trajectory,
    diffusivity,
    adjoint_end,
    obs_jac,
    obs_value,
    obs_weight,
    obs_valid,
    obs_owner,
    obs_tile,
):
    devices = lax.axis_size("tm") * lax.axis_size("lat")
    blocks = obs_owner.shape[0]
    slots = max(2, 2 * blocks // devices)
    rounded = sweep(
        obs_owner[:, 0][None, :], obs_tile[None, :], obs_value, obs_weight, obs_valid,
        trajectory, diffusivity, adjoint_end, obs_jac, slots,
    )
    return widen(rounded)


def solution(mesh):
    in_specs = (
        P("tm", "lat", None, None),
        P("tm", "lat", None, None),
        P("lat", None, None),
        P(("tm", "lat"), None, None),
        P(("tm", "lat"), None),
        P(("tm", "lat"), None),
        P(("tm", "lat"), None),
        P(("tm", "lat"), None),
        P(("tm", "lat")),
    )
    out_specs = P("tm", "lat", None, None)
    return jax.shard_map(
        per_device, mesh=mesh, in_specs=in_specs, out_specs=out_specs, check_vma=False
    )
```

```python
import functools

import jax
import jax.numpy as jnp
from jax import lax
from jax.experimental import pallas as pl
from jax.experimental.pallas import tpu as pltpu
from jax.sharding import PartitionSpec as P

TW = 2
SUB = 2
LANES = 128
PAD = 8
CHUNK = 8
SCALE = 2.0**17
MESH = pl.DeviceIdType.MESH
VMEM = pl.BlockSpec(memory_space=pltpu.VMEM)


def split(x):
    top = x.astype(jnp.bfloat16)
    return top, (x - top.astype(jnp.float32)).astype(jnp.bfloat16)


def dot(a, b):
    return jnp.dot(a, b, preferred_element_type=jnp.float32)


def iota(shape, axis):
    return lax.broadcasted_iota(jnp.int32, shape, axis)


def ones_where(mask):
    return jnp.where(mask, 1.0, 0.0)


def sweep_kernel(
    lats, sections, slots,
    owner_hbm, tile_hbm, value_hbm, weight_hbm, valid_hbm, traj_hbm, coeff_hbm, end_hbm, jac_hbm,
    out_ref,
    owner_ref, tile_ref, value_ref, weight_ref, valid_ref, traj, coeff, jac, jac_t, fields, chosen, place, place_t, which, pair,
    ids_out, ids_in, state_out, state_in, term_out, term_in, state_rows, resid_rows, terms, terms_t,
    coded, kappa, kappa_low, kappa_high, main, forcing, weighted, partial, second, early,
    edge_low, edge_high, low, high,
    load_sem, end_sem, ids_send, ids_recv, state_send, state_recv, term_send, term_recv,
    kappa_send, kappa_recv, down_send, down_recv, up_send, up_recv,
    low_send, low_recv, high_send, high_recv, out_send, out_recv, own_sem,
):
    section, band = lax.axis_index("tm"), lax.axis_index("lat")
    count = sections * lats
    me = section * lats + band
    rows, levels, nlon = coeff.shape
    blocks = owner_ref.shape[1]
    total = count * PAD
    columns = nlon // LANES
    per_column = LANES // TW
    tile_len = levels * TW
    part = levels // sections
    chunks = part // CHUNK
    width = part * TW
    has_low, has_high = band > 0, band < lats - 1
    last = sections - 1

    loads = [
        pltpu.make_async_copy(src, dst, load_sem.at[i])
        for i, (src, dst) in enumerate(
            (
                (owner_hbm, owner_ref), (tile_hbm, tile_ref), (coeff_hbm.at[0], coeff), (traj_hbm.at[0], traj),
                (jac_hbm, jac), (value_hbm, value_ref), (weight_hbm, weight_ref), (valid_hbm, valid_ref),
            )
        )
    ]
    for load in loads:
        load.start()

    def end_load(c):
        at = pl.multiple_of(section * part + c * CHUNK, CHUNK)
        return pltpu.make_async_copy(end_hbm.at[:, pl.ds(at, CHUNK), :], main.at[sections, c], end_sem.at[c])

    for c in range(chunks):
        end_load(c).start()

    barrier = pltpu.get_barrier_semaphore()

    def peer(j):
        to = lax.rem(me + j, count)
        return to, (to // lats, lax.rem(to, lats))

    def nearer(i):
        far = lats - 1 - i // 2
        lat = jnp.where(lax.rem(i, 2) == 0, band + far, band - far)
        return far, lat, (lat >= 0) & (lat < lats) & ((far > 0) | (lax.rem(i, 2) == 0))

    def greet(i, carry):
        far, lat, inside = nearer(i)

        @pl.when(inside)
        def _():
            def one(j, carry):
                where = (lax.rem(section + sections - j, sections), lat)
                pl.semaphore_signal(barrier, inc=1, device_id=where, device_id_type=MESH)
                return carry

            lax.fori_loop(1, jnp.where(far > 0, sections + 1, sections), one, 0)

        return carry

    lax.fori_loop(0, 2 * lats, greet, 0)

    def remote(src, dst, send, recv, where):
        return pltpu.make_async_remote_copy(
            src_ref=src, dst_ref=dst, send_sem=send, recv_sem=recv, device_id=where, device_id_type=MESH
        )

    def swap(pick, into, send, recv, used):
        def outgoing(to):
            where = (to // lats, lax.rem(to, lats))
            return remote(pick(to).at[:used], into.at[me, :used], send.at[to], recv.at[me], where)

        def incoming(source):
            where = (source // lats, lax.rem(source, lats))
            return remote(pick(source).at[:used], into.at[source, :used], send.at[source], recv.at[source], where)

        def launch(i, carry):
            far, lat, inside = nearer(i)

            @pl.when(inside)
            def _():
                def one(j, carry):
                    outgoing(lax.rem(section + sections - j, sections) * lats + lat).start()
                    return carry

                lax.fori_loop(1, jnp.where(far > 0, sections + 1, sections), one, 0)

            return carry

        def land(j, carry):
            incoming(lax.rem(me + count - j, count)).wait_recv()
            return carry

        def drain(j, carry):
            outgoing(lax.rem(me + j, count)).wait_send()
            return carry

        def begin():
            lax.fori_loop(0, 2 * lats, launch, 0)
            into[me] = pick(me)[...]

        return begin, lambda: lax.fori_loop(1, count, land, 0), lambda: lax.fori_loop(1, count, drain, 0)

    ids_begin, ids_land, ids_drain = swap(lambda d: ids_out.at[lax.rem(d, lats)], ids_in, ids_send, ids_recv, 1)
    state_begin, state_land, state_drain = swap(lambda d: state_out.at[d], state_in, state_send, state_recv, slots)
    term_begin, term_land, term_drain = swap(lambda d: term_out.at[d], term_in, term_send, term_recv, slots)

    for load in loads[:2]:
        load.wait()
    owner = owner_ref[...]
    mine = owner == iota((count, blocks), 0)
    before = ones_where(iota((blocks, blocks), 0) < iota((blocks, blocks), 1)).astype(jnp.bfloat16)
    rank = dot(ones_where(mine).astype(jnp.bfloat16), before)
    target = jnp.where(mine, iota((count, blocks), 0).astype(jnp.float32) * PAD + rank, 0.0)
    slot = jnp.sum(target, axis=0, keepdims=True)
    tile = tile_ref[...]
    column = (tile // per_column + 1).astype(jnp.float32)
    inside = lax.rem(tile, per_column).astype(jnp.float32)
    lane = iota((count, LANES), 1)
    packed = jnp.zeros((count, LANES), jnp.float32)
    for s in range(slots):
        here = mine & (rank == float(s))
        for at, what in ((s, column), (PAD + s, inside)):
            found = jnp.sum(jnp.where(here, what, 0.0), axis=1, keepdims=True)
            packed = jnp.where(lane == at, found, packed)
    lists = packed[:lats]
    for s in range(1, sections):
        lists = lists + pltpu.roll(packed[s * lats : (s + 1) * lats], s * 2 * PAD, 1)
    for b in range(lats):
        ids_out[b] = lists[b : b + 1]
    state_in[...] = jnp.zeros_like(state_in)
    term_in[...] = jnp.zeros_like(term_in)
    pl.semaphore_wait(barrier, count - 1)
    ids_begin()

    def kappa_copy(j):
        to = lax.rem(section + j, sections)
        return remote(coded.at[to], kappa.at[section], kappa_send.at[j], kappa_recv.at[j], (to, band))

    def kappa_arrival(j):
        source = lax.rem(section + sections - j, sections)
        return remote(coded.at[source], kappa.at[source], kappa_send.at[j], kappa_recv.at[j], (source, band))

    def row_down(j):
        to = lax.rem(section + j, sections)
        return remote(coded.at[to, :, 0], kappa_high.at[section], down_send.at[j], down_recv.at[j], (to, band - 1))

    def row_up(j):
        to = lax.rem(section + j, sections)
        return remote(coded.at[to, :, rows - 1], kappa_low.at[section], up_send.at[j], up_recv.at[j], (to, band + 1))

    def from_high(j):
        source = lax.rem(section + sections - j, sections)
        return remote(coded.at[source, :, 0], kappa_high.at[source], down_send.at[j], down_recv.at[j], (source, band))

    def from_low(j):
        source = lax.rem(section + sections - j, sections)
        return remote(coded.at[source, :, 0], kappa_low.at[source], up_send.at[j], up_recv.at[j], (source, band))

    def share_kappa():
        for j in range(sections - 1, 0, -1):
            kappa_copy(j).start()

    def share_rows(first, stop):
        @pl.when(has_low)
        def _():
            for j in range(first, stop):
                row_down(j).start()

        @pl.when(has_high)
        def _():
            for j in range(first, stop):
                row_up(j).start()

    loads[2].wait()

    def encode(q, carry):
        for c in range(chunks):
            at = pl.multiple_of(q * part + c * CHUNK, CHUNK)
            for r in range(rows):
                scaled = coeff[r, pl.ds(at, CHUNK), :] * SCALE + 0.5
                coded[q, c, r] = scaled.astype(jnp.int32).astype(jnp.int16)
        return carry

    lax.fori_loop(0, sections, encode, 0)
    is_odd = lax.rem(section, 2) == lax.rem(last, 2)

    @pl.when(is_odd)
    def _():
        share_kappa()
        share_rows(0, sections)

    @pl.when(jnp.logical_not(is_odd))
    def _():
        share_rows(0, 1)

    kappa[section] = coded[section]

    holds = ones_where(iota((total, blocks), 0).astype(jnp.float32) == slot)
    place[...] = holds.astype(jnp.bfloat16)
    place_t[...] = holds.T.astype(jnp.bfloat16)

    @pl.when(jnp.logical_not(has_low))
    def _():
        low[...] = jnp.zeros_like(low)
        kappa_low[...] = jnp.zeros_like(kappa_low)

    @pl.when(jnp.logical_not(has_high))
    def _():
        high[...] = jnp.zeros_like(high)
        kappa_high[...] = jnp.zeros_like(kappa_high)

    order = iota((tile_len, tile_len), 0)
    other = iota((tile_len, tile_len), 1)

    def by_part(a, b, size):
        level = a // TW
        place_of = (level // size) * (size * TW) + lax.rem(a, TW) * size + lax.rem(level, size)
        return ones_where(place_of == b).astype(jnp.bfloat16)

    to_parts, from_parts = by_part(order, other, part), by_part(other, order, levels)

    loads[3].wait()
    even = lax.rem(iota((levels, nlon), 1), TW)

    def field(r, carry):
        values = traj[r]
        top = values.astype(jnp.bfloat16).astype(jnp.float32)
        parts = [jnp.where(even == p, x, 0.0) for x in (top, values - top) for p in range(TW)]
        stack = jnp.concatenate(parts, axis=0).T.astype(jnp.bfloat16)
        fields[r] = jnp.concatenate(
            [dot(stack[:, :tile_len], from_parts), dot(stack[:, tile_len:], from_parts)], axis=1
        ).astype(jnp.bfloat16)
        return carry

    lax.fori_loop(0, rows, field, 0)

    ids_land()
    ids = jnp.concatenate([ids_in[d] for d in range(count)], axis=0).astype(jnp.bfloat16)
    source = ones_where(iota((total, count), 0) // PAD == iota((total, count), 1)).astype(jnp.bfloat16)
    spread = dot(source, ids)
    nth = lax.rem(iota((total, LANES), 0), PAD)
    lanes = iota((total, LANES), 1)

    def listed(s):
        at = nth + s * 2 * PAD
        outer = jnp.sum(jnp.where(lanes == at, spread, 0.0), axis=1, keepdims=True)
        inner = jnp.sum(jnp.where(lanes == at + PAD, spread, 0.0), axis=1, keepdims=True)
        which[s] = jnp.broadcast_to(outer, (total, LANES)).astype(jnp.bfloat16)
        pair[s] = ones_where((lanes // TW).astype(jnp.float32) == inner).astype(jnp.bfloat16)

    nothing = jnp.zeros((total, LANES), jnp.bfloat16)

    def tiles(s, r, c):
        return jnp.where(which[s] == jnp.bfloat16(r * columns + c + 1), pair[s], nothing)

    listed(section)
    gathered = jnp.zeros((total, 2 * tile_len), jnp.float32)
    for r in range(rows):
        for c in range(columns):
            chosen[r, :, c * LANES : (c + 1) * LANES] = tiles(section, r, c)
        gathered = gathered + dot(chosen[r], fields[r])
    states = gathered[:, :tile_len] + gathered[:, tile_len:]
    state_out[...] = states.reshape(count, PAD, tile_len)
    state_begin()

    @pl.when(jnp.logical_not(is_odd))
    def _():
        share_kappa()
        share_rows(1, sections)

    for load in loads[4:]:
        load.wait()

    def turn(k, carry):
        jac_t[k] = jac[k].astype(jnp.float32).T.astype(jnp.bfloat16)
        return carry

    lax.fori_loop(0, blocks, turn, 0, unroll=4)

    def downward(s, c):
        return remote(edge_low.at[s, c], high.at[s, c], low_send.at[s, c], high_recv.at[s, c], (section, band - 1))

    def upward(s, c):
        return remote(edge_high.at[s, c], low.at[s, c], high_send.at[s, c], low_recv.at[s, c], (section, band + 1))

    def along(mid):
        return pltpu.roll(mid, 1, 1) + pltpu.roll(mid, nlon - 1, 1) - 4.0 * mid

    def decode(x):
        return x.astype(jnp.int32).astype(jnp.float32) * (1.0 / SCALE)

    def begin(s, c, steps=(0, 1, 2)):
        end = rows - 1

        def weigh(r):
            weighted[c, r] = decode(kappa[s, c, r]) * main[s + 1, c, r].astype(jnp.float32)

        def inner(r):
            value = main[s + 1, c, r].astype(jnp.float32) + along(weighted[c, r])
            if r > 0:
                value = value + weighted[c, r - 1]
            if r < end:
                value = value + weighted[c, r + 1]
            partial[c, r] = value

        for step, r, near, ref, there, copy in (
            (0, 0, 1, edge_low, has_low, downward), (1, end, end - 1, edge_high, has_high, upward)
        ):
            if step not in steps:
                continue
            weigh(r)
            weigh(near)
            inner(r)
            ref[s, c, 0] = weighted[c, r].astype(jnp.bfloat16)
            ref[s, c, 1] = (decode(kappa[s, c, r]) * partial[c, r]).astype(jnp.bfloat16)

            @pl.when(there)
            def _(copy=copy):
                copy(s, c).start()

        if 2 not in steps:
            return
        for r in range(2, end - 1):
            weigh(r)
        for r in range(1, end):
            inner(r)

    def complete(s, c, store):
        @pl.when(has_low)
        def _():
            upward(s, c).wait_recv()

        @pl.when(has_high)
        def _():
            downward(s, c).wait_recv()

        end = rows - 1
        partial[c, 0] = partial[c, 0] + low[s, c, 0].astype(jnp.float32)
        partial[c, end] = partial[c, end] + high[s, c, 0].astype(jnp.float32)
        second[0] = low[s, c, 1].astype(jnp.float32) + decode(kappa_low[s, c]) * weighted[c, 0]
        second[rows + 1] = high[s, c, 1].astype(jnp.float32) + decode(kappa_high[s, c]) * weighted[c, end]
        for r in range(rows):
            second[r + 1] = decode(kappa[s, c, r]) * partial[c, r]
        for r in range(rows):
            store(r, partial[c, r] + second[r] + second[r + 2] + along(second[r + 1]))

    def spot(q, c, r):
        return out_ref.at[r, pl.ds(pl.multiple_of(q * part + c * CHUNK, CHUNK), CHUNK), :]

    def give(s, c, r):
        where = (s, band)
        return remote(main.at[s, c, r], spot(section, c, r), out_send.at[s, c, r], out_recv.at[section, c, r], where)

    def taken(q, c, r):
        return remote(main.at[q, c, r], spot(q, c, r), out_send.at[q, c, r], out_recv.at[q, c, r], (q, band))

    def keep_own(c, r):
        return pltpu.make_async_copy(main.at[section, c, r], spot(section, c, r), own_sem.at[c, r])

    def finish(s, c, r, value):
        main[s, c, r] = value.astype(jnp.bfloat16)

    def deliver(s, c):
        @pl.when(s != section)
        def _():
            for r in range(rows):
                give(s, c, r).start()

        @pl.when(s == section)
        def _():
            for r in range(rows):
                keep_own(c, r).start()

    last_from = lax.rem(section + 1, sections)

    @pl.when(last_from != 0)
    def _():
        kappa_arrival(last_from).wait_recv()

    for c in range(chunks):
        end_load(c).wait()

    def open_last(c, carry):
        begin(last, c)
        return carry

    lax.fori_loop(0, chunks, open_last, 0)

    state_land()
    top, rest = split(state_in[...].reshape(total, tile_len))
    top, rest = dot(place_t[...], top), dot(place_t[...], rest)
    groups = blocks // PAD
    for g in range(groups):
        span = slice(g * PAD, (g + 1) * PAD)
        state_rows[g] = jnp.concatenate([top[span], rest[span]], axis=0).astype(jnp.bfloat16)
    among = lax.rem(iota((2 * PAD, tile_len), 0), PAD)

    def product(both, mats, g):
        picked = jnp.zeros((2 * PAD, tile_len), jnp.float32)
        for i in range(0, PAD, 2):
            k = g * PAD + i
            full = dot(both, jnp.concatenate([mats[k], mats[k + 1]], axis=1))
            picked = jnp.where(among == i, full[:, :tile_len], picked)
            picked = jnp.where(among == i + 1, full[:, tile_len:], picked)
        return picked[:PAD] + picked[PAD:]

    for g in range(groups):
        here = slice(g * PAD, (g + 1) * PAD)
        pred = product(state_rows[g], jac_t, g)
        weight = weight_ref[here, :] * valid_ref[here, :].astype(jnp.float32)
        resid = weight * (value_ref[here, :] - pred)
        top = resid.astype(jnp.bfloat16).astype(jnp.float32)
        resid_rows[g] = jnp.concatenate([top, resid - top], axis=0).astype(jnp.bfloat16)
    for g in range(groups):
        terms[g * PAD : (g + 1) * PAD, :] = product(resid_rows[g], jac, g)
    top, rest = split(terms[...])
    top, rest = dot(top, to_parts).astype(jnp.bfloat16), dot(rest, to_parts).astype(jnp.bfloat16)
    sent = dot(place[...], top) + dot(place[...], rest)
    group = lats * PAD
    strip = iota((group, tile_len), 1) // width
    for q in range(sections):
        parcel = jnp.zeros((group, tile_len), jnp.float32)
        for s in range(sections):
            moved = sent[s * group : (s + 1) * group]
            if s != q:
                moved = pltpu.roll(moved, ((s - q) % sections) * width, 1)
            parcel = jnp.where(strip == s, moved, parcel)
        term_out[q * lats : (q + 1) * lats] = parcel.reshape(lats, PAD, tile_len)
    term_begin()
    def list_other(j, carry):
        listed(lax.rem(section + j, sections))
        return carry

    lax.fori_loop(1, sections, list_other, 0)

    ids_drain()
    state_drain()

    for j in range(sections):
        @pl.when(has_high)
        def _(j=j):
            from_high(j).wait_recv()

        @pl.when(has_low)
        def _(j=j):
            from_low(j).wait_recv()

    def kappa_land(j, carry):
        @pl.when(j != last_from)
        def _():
            kappa_arrival(j).wait_recv()

        return carry

    lax.fori_loop(1, sections, kappa_land, 0)

    def close_last(c, carry):
        def keep(r, value):
            early[c, r] = value

        complete(last, c, keep)
        return carry

    lax.fori_loop(0, chunks, close_last, 0)

    term_land()
    got = term_in[...].reshape(total, tile_len).T
    top = got.astype(jnp.bfloat16).astype(jnp.float32)
    rest = got - top
    for s in range(sections):
        span = slice(s * width, (s + 1) * width)
        stack = jnp.concatenate([top[span], rest[span]], axis=0).astype(jnp.bfloat16)
        terms_t[s] = stack
    wide = 2 * LANES
    parity = lax.rem(iota((part, wide), 1), TW)

    def scatter(s, some):
        left = terms_t[s]
        for r in some:
            for c in range(nlon // wide):
                right = jnp.concatenate([tiles(s, r, 2 * c), tiles(s, r, 2 * c + 1)], axis=1)
                both = dot(left, right)
                both = both[:width] + both[width:]
                value = jnp.where(parity == 0, both[:part], both[part:])
                for k in range(chunks):
                    forcing[s, k, r, :, c * wide : (c + 1) * wide] = value[k * CHUNK : (k + 1) * CHUNK]

    half = rows // 2
    for some, steps in ((range(half), (0,)), (range(half, rows), (1, 2))):
        scatter(last, some)

        def start_last(c, carry, some=some, steps=steps):
            for r in some:
                finish(last, c, r, early[c, r] + forcing[last, c, r])
            if last > 0:
                begin(last - 1, c, steps)
            return carry

        lax.fori_loop(0, chunks, start_last, 0)

    def give_last(c, carry):
        deliver(last, c)
        return carry

    lax.fori_loop(0, chunks, give_last, 0)

    def scatter_other(j, carry):
        scatter(last - j, range(rows))
        return carry

    lax.fori_loop(1, sections, scatter_other, 0)

    def go(i, carry):
        s = last - 1 - i // chunks
        c = lax.rem(i, chunks)
        complete(s, c, lambda r, value: finish(s, c, r, value + forcing[s, c, r]))

        @pl.when(s > 0)
        def _():
            begin(s - 1, c)

        deliver(s, c)
        return carry

    lax.fori_loop(0, last * chunks, go, 0)

    term_drain()
    for j in range(1, sections):
        kappa_copy(j).wait_send()
    for cond, copy in ((has_low, row_down), (has_high, row_up)):
        @pl.when(cond)
        def _(copy=copy):
            for j in range(sections):
                copy(j).wait_send()

    def settle(i, carry):
        s, c = i // chunks, lax.rem(i, chunks)

        @pl.when(has_low)
        def _():
            downward(s, c).wait_send()

        @pl.when(has_high)
        def _():
            upward(s, c).wait_send()

        @pl.when(s != section)
        def _():
            for r in range(rows):
                give(s, c, r).wait_send()

        @pl.when(s == section)
        def _():
            for r in range(rows):
                keep_own(c, r).wait()

        return carry

    lax.fori_loop(0, sections * chunks, settle, 0)

    def gain(i, carry):
        q, c = lax.rem(section + 1 + i // chunks, sections), lax.rem(i, chunks)
        for r in range(rows):
            taken(q, c, r).wait_recv()
        return carry

    lax.fori_loop(0, last * chunks, gain, 0)


def sweep(owner, tile, value, weight, valid, traj, coeff, end, jac, slots):
    lats, sections = lax.axis_size("lat"), lax.axis_size("tm")
    count = sections * lats
    _, rows, levels, nlon = traj.shape
    blocks = owner.shape[1]
    tile_len = levels * TW
    total = count * PAD
    chunks = levels // sections // CHUNK
    bf16, f32 = jnp.bfloat16, jnp.float32
    parcels = pltpu.VMEM((count, PAD, tile_len), f32)
    stacked = pltpu.VMEM((blocks // PAD, 2 * PAD, tile_len), bf16)
    work = pltpu.VMEM((chunks, rows, CHUNK, nlon), f32)
    edges = pltpu.VMEM((sections, chunks, SUB, CHUNK, nlon), bf16)
    codes = lambda *lead: pltpu.VMEM(lead + (CHUNK, nlon), jnp.int16)
    hbm = pl.BlockSpec(memory_space=pltpu.HBM)
    dma = pltpu.SemaphoreType.DMA
    return pl.pallas_call(
        functools.partial(sweep_kernel, lats, sections, slots),
        out_shape=jax.ShapeDtypeStruct((rows, levels, nlon), bf16),
        in_specs=[hbm] * 9,
        out_specs=hbm,
        scratch_shapes=[
            pltpu.VMEM(owner.shape, owner.dtype),
            pltpu.VMEM(tile.shape, tile.dtype),
            pltpu.VMEM(value.shape, value.dtype),
            pltpu.VMEM(weight.shape, weight.dtype),
            pltpu.VMEM(valid.shape, valid.dtype),
            pltpu.VMEM((rows, levels, nlon), f32),
            pltpu.VMEM((rows, levels, nlon), f32),
            pltpu.VMEM(jac.shape, bf16),
            pltpu.VMEM(jac.shape, bf16),
            pltpu.VMEM((rows, nlon, 2 * tile_len), bf16),
            pltpu.VMEM((rows, total, nlon), bf16),
            pltpu.VMEM((total, blocks), bf16),
            pltpu.VMEM((blocks, total), bf16),
            pltpu.VMEM((sections, total, LANES), bf16),
            pltpu.VMEM((sections, total, LANES), bf16),
            pltpu.VMEM((lats, 1, LANES), f32),
            pltpu.VMEM((count, 1, LANES), f32),
            parcels, parcels, parcels, parcels, stacked, stacked,
            pltpu.VMEM((blocks, tile_len), f32),
            pltpu.VMEM((sections, 2 * tile_len // sections, total), bf16),
            codes(sections, chunks, rows),
            codes(sections, chunks, rows),
            codes(sections, chunks),
            codes(sections, chunks),
            pltpu.VMEM((sections + 1, chunks, rows, CHUNK, nlon), bf16),
            pltpu.VMEM((sections, chunks, rows, CHUNK, nlon), f32),
            work, work,
            pltpu.VMEM((rows + 2, CHUNK, nlon), f32),
            work,
            edges, edges, edges, edges,
            dma((8,)),
            dma((chunks,)),
        ]
        + [dma((count,))] * 6
        + [dma((sections,))] * 6
        + [dma((sections, chunks))] * 4
        + [dma((sections, chunks, rows))] * 2
        + [dma((chunks, rows))],
        compiler_params=pltpu.CompilerParams(
            collective_id=1, has_side_effects=True, vmem_limit_bytes=63 * 1024 * 1024
        ),
        name="sweep",
    )(owner, tile, value, weight, valid, traj, coeff, end, jac)


def widen_kernel(x_hbm, out_hbm, x, wide, in_sem, out_sem):
    rows = x.shape[0]

    def load(r):
        return pltpu.make_async_copy(x_hbm.at[r], x.at[r], in_sem.at[r])

    def save(r):
        return pltpu.make_async_copy(wide.at[r], out_hbm.at[0, r], out_sem.at[r])

    for r in range(rows):
        load(r).start()
    for r in range(rows):
        load(r).wait()
        wide[r] = x[r].astype(jnp.float32)
        save(r).start()
    for r in range(rows):
        save(r).wait()


def widen(x):
    hbm = pl.BlockSpec(memory_space=pltpu.HBM)
    dma = pltpu.SemaphoreType.DMA((x.shape[0],))
    return pl.pallas_call(
        widen_kernel,
        out_shape=jax.ShapeDtypeStruct((1,) + x.shape, jnp.float32),
        in_specs=[hbm],
        out_specs=hbm,
        scratch_shapes=[pltpu.VMEM(x.shape, x.dtype), pltpu.VMEM(x.shape, jnp.float32), dma, dma],
        compiler_params=pltpu.CompilerParams(vmem_limit_bytes=63 * 1024 * 1024),
        name="widen",
    )(x)


def per_device(
    trajectory,
    diffusivity,
    adjoint_end,
    obs_jac,
    obs_value,
    obs_weight,
    obs_valid,
    obs_owner,
    obs_tile,
):
    devices = lax.axis_size("tm") * lax.axis_size("lat")
    blocks = obs_owner.shape[0]
    slots = max(2, 2 * blocks // devices)
    rounded = sweep(
        obs_owner[:, 0][None, :], obs_tile[None, :], obs_value, obs_weight, obs_valid,
        trajectory, diffusivity, adjoint_end, obs_jac, slots,
    )
    return widen(rounded)


def solution(mesh):
    in_specs = (
        P("tm", "lat", None, None),
        P("tm", "lat", None, None),
        P("lat", None, None),
        P(("tm", "lat"), None, None),
        P(("tm", "lat"), None),
        P(("tm", "lat"), None),
        P(("tm", "lat"), None),
        P(("tm", "lat"), None),
        P(("tm", "lat")),
    )
    out_specs = P("tm", "lat", None, None)
    return jax.shard_map(
        per_device, mesh=mesh, in_specs=in_specs, out_specs=out_specs, check_vma=False
    )
```
